32 devices in a mesh: dp: 8 (over z, y), ep: 4 (over x, core).
Axes of the slice: x: 2, y: 2, z: 4, core: 2. Of those that a mesh axis runs over, the one named last changes fastest.
Arguments:
- tokens: bfloat16 [128, 4096], P(('dp', 'ep')), may hold values from -6 to 6
- router: float32 [4096, 8], replicated, may hold values from -0.1875 to 0.1875
- expert_ids: int32 [128, 2], P(('dp', 'ep')), may hold values from 0 to 7, all different within a row; in each aligned block of 4 rows (0 to 3, 4 to 7, ...) at most 2 rows name the same one
- w_gate: bfloat16 [8, 4096, 12288], P('dp', None, 'ep'), may hold values from -0.09375 to 0.09375
- w_up: bfloat16 [8, 4096, 12288], P('dp', None, 'ep'), may hold values from -0.09375 to 0.09375
- w_down: bfloat16 [8, 12288, 4096], P('dp', 'ep'), may hold values from -0.0546875 to 0.0546875
- states: bfloat16 [128, 16, 8192], P('dp', None, 'ep'), may hold values from -6 to 6
- kv_blocks: bfloat16 [256, 2, 16, 1024], P('dp', None, None, 'ep'), may hold values from -6 to 6
- plan_slots: int32 [8, 2, 3], replicated, may hold values from -1 to 15, as said below
- plan_len: int32 [8, 2], replicated, may hold values from 0 to 32, as said below
- plan_blocks: int32 [8, 2, 2, 2], replicated, may hold values from -1 to 31, as said below
Outputs:
- mixed: bfloat16 [128, 4096], P(('dp', 'ep'))
- new_states: bfloat16 [128, 16, 8192], P('dp', None, 'ep')
- new_cache: bfloat16 [256, 2, 16, 1024], P('dp', None, None, 'ep')
The draws below stay inside these ranges and needn't reach their ends.
Inputs may be any that keep to these rules, and one draw needn't show every extreme that they name: `expert_ids`: in the rows of one device no expert is named more than 2 times. `plan_slots`: A move is live exactly where its first entry is not -1, and then all three entries are set; otherwise all are -1. For each m there is one distance d_m from 1 to 7, distinct for distinct m, such that every live move (r, m) goes to rank (r + d_m) mod 8. The leaving slots of a rank are distinct, the slots taken at a rank are distinct and differ from its leaving slots. Some rank has all 2 moves live. `plan_len`: zero exactly where the move is not live; some move holds 32 tokens. `plan_blocks`: entry j of both tables is -1 exactly where j * 16 >= plan_len. The blocks leaving a rank are distinct, the blocks taken at a rank are distinct and differ from the ones leaving it.
All inputs are finite; a program needn't handle non-finite values.
Results may differ from the reference program's by a relative error of at most 0.005.
Values may be sent and summed in bfloat16 or wider, within the bound.
A program may use at most 128 MiB of HBM per device.

```python
import math
import jax
import jax.numpy as jnp
import numpy as np
from jax import lax

D = 4096
FF = 12288
EXPERTS = 8
CHANNELS = 8192
NST = 16
KVH = 8
HEAD = 128
BLK = 16
TOK_DEV = 4
SLOTS = 16
BLOCKS = 32
MOVE = 2
BPR = 2
CAP = 2
GROUP = 1
TOKENS = 128
N_DP = 8
N_EP = 4


def plan_core(key):
    base = jax.random.fold_in(key, 4242)
    keys = jax.random.split(base, 7)
    offsets = 1 + jax.random.permutation(keys[1], N_DP - 1)[:MOVE]
    rank_line = jnp.arange(N_DP, dtype=jnp.int32)
    target_rank = ((rank_line[:, None] + offsets[None, :]) % N_DP).astype(jnp.int32)
    move_line = jnp.arange(MOVE, dtype=jnp.int32)
    live = jax.random.randint(keys[2], (N_DP, MOVE), 0, 5) < 3
    busiest = jax.random.randint(keys[3], (), 0, N_DP)
    live = live | (rank_line[:, None] == busiest)
    slot_perm = jax.vmap(lambda inner: jax.random.permutation(inner, SLOTS))(jax.random.split(keys[4], N_DP))
    block_perm = jax.vmap(lambda inner: jax.random.permutation(inner, BLOCKS))(jax.random.split(keys[5], N_DP))
    length = jax.random.randint(keys[6], (N_DP, MOVE), 1, BPR * BLK + 1)
    longest = (rank_line[:, None] == busiest) & (move_line[None, :] == 0)
    length = jnp.where(longest, BPR * BLK, length)
    length = jnp.where(live, length, 0).astype(jnp.int32)
    leaving_slot = jnp.where(live, slot_perm[:, :MOVE], -1)
    taken_slot = jnp.where(live, slot_perm[target_rank, MOVE + move_line[None, :]], -1)
    drawn_rank = jnp.where(live, target_rank, -1)
    plan_slots = jnp.stack([leaving_slot, drawn_rank, taken_slot], axis=-1).astype(jnp.int32)
    block_count = (length + BLK - 1) // BLK
    block_line = jnp.arange(BPR, dtype=jnp.int32)
    used = block_line[None, None, :] < block_count[:, :, None]
    leaving_block = block_perm[:, :MOVE * BPR].reshape(N_DP, MOVE, BPR)
    taken_block = block_perm[target_rank[:, :, None], MOVE * BPR + move_line[None, :, None] * BPR + block_line[None, None, :]]
    leaving_block = jnp.where(used, leaving_block, -1)
    taken_block = jnp.where(used, taken_block, -1)
    plan_blocks = jnp.stack([leaving_block, taken_block], axis=2).astype(jnp.int32)
    return (plan_slots, length, plan_blocks)


def draw_plan_slots(key, part):
    return plan_core(key)[0]


def draw_plan_len(key, part):
    return plan_core(key)[1]


def draw_plan_blocks(key, part):
    return plan_core(key)[2]


def levels(own_key, dims, shards, smallest, high):
    factor_of = 1.0
    for axis_at, shards_of in shards:
        draws = jax.random.uniform(jax.random.fold_in(jax.random.fold_in(own_key, 6), axis_at), (shards_of,), jnp.float32, smallest / len(shards), high / len(shards))
        factor_of = factor_of * jnp.repeat(jnp.exp(draws), dims[axis_at] // shards_of).reshape((-1,) + (1,) * (len(dims) - 1 - axis_at))
    return factor_of


def shared_out(key, own, number, rows, count, top, reach, skew):
    order = jax.random.permutation(key, count)
    heavy_load, usual = shares(count, rows * top, reach, skew, True), shares(count, rows * top, reach, skew, False)
    places = jnp.arange(count)

    def named(sizes, rotation):
        used = int((sizes > 0).sum())
        fixed = max(1, used // 4)
        passed = fixed + (places - fixed + rotation * (used - fixed)) % max(1, count - fixed)
        return jnp.zeros((count,), jnp.int32).at[order[jnp.where(places < fixed, places, passed)]].set(jnp.asarray(sizes, jnp.int32))

    sizes = jnp.where(number % 4 == 0, named(heavy_load, number // 4), named(usual, number - number // 4 - 1))
    mixed = jax.random.permutation(jax.random.fold_in(own, 3), count)
    giver, taker = mixed[0:count // 2 * 2:2], mixed[1:count // 2 * 2:2]
    margin = jnp.minimum(sizes[giver] - 1, reach - sizes[taker]) // 2
    margin = jnp.where((giver == order[0]) | (taker == order[0]) | (sizes[taker] == 0), 0, jnp.maximum(margin, 0))
    passed = jax.random.randint(jax.random.fold_in(own, 4), (count // 2,), 0, 1 << 20) % (margin + 1)
    sizes = sizes.at[giver].add(-passed).at[taker].add(passed)
    labels = jnp.searchsorted(jnp.cumsum(sizes), jnp.arange(rows * top), side="right").astype(jnp.int32)
    listing = labels.reshape(top, rows).T
    listing = listing[jax.random.permutation(jax.random.fold_in(own, 1), rows)]
    rotation = jax.random.randint(jax.random.fold_in(own, 2), (rows, 1), 0, top)
    return jnp.take_along_axis(listing, (jnp.arange(top)[None, :] + rotation) % top, axis=1)


def shares(number_of, total, reach, skew, full):
    weights = [(1 << 20) // math.isqrt(rank ** skew) + 1 for rank in range(1, number_of + 1)]
    largest = reach if full else min(reach, max(-(-total // number_of), total * weights[0] // sum(weights)))
    least = 1 if total - largest >= number_of - 1 else 0
    holding, rest = [largest] + [least] * (number_of - 1), total - largest - least * (number_of - 1)
    while rest > 0:
        movable = [i for i in range(1, number_of) if holding[i] < largest] or [i for i in range(1, number_of) if holding[i] < reach]
        whole, left = sum([weights[i] for i in movable]), rest
        for i in movable:
            addition = min(reach - holding[i], max(1, left * weights[i] // whole), rest)
            holding[i] = holding[i] + addition
            rest = rest - addition
    return np.array(holding)


def bell_draw(rng, shape, scale, limit, pieces=(), held_as=jnp.bfloat16):
    values = scale * jax.random.normal(rng, shape, jnp.float32)
    if pieces:
        values = values * levels(rng, shape, pieces, -0.22, 0.18)
    return jnp.clip(values, -limit, limit).astype(held_as)


def setup_inputs(seed: int = 0) -> dict:
    streams_of = jax.random.split(jax.random.key(seed), 12)
    tokens = bell_draw(streams_of[0], (TOKENS, D), 1.0, 6.0, ((0, 32),))
    router = bell_draw(streams_of[1], (D, EXPERTS), (D // 4) ** -0.5, 0.1875, (), jnp.float32)
    expert_ids_keys = jax.random.split(jax.random.fold_in(streams_of[2], 1), TOKENS // TOK_DEV)
    expert_ids_turns = jax.random.permutation(jax.random.fold_in(streams_of[2], 3), TOKENS // TOK_DEV)
    expert_ids = jax.vmap(lambda own, number: shared_out(jax.random.fold_in(streams_of[2], 2), own, number, TOK_DEV, EXPERTS, 2, CAP, 2))(expert_ids_keys, expert_ids_turns).reshape((TOKENS, 2))
    w_gate = bell_draw(streams_of[3], (EXPERTS * GROUP, D, FF // GROUP), D ** -0.5, 0.09375, ((0, 8), (2, 4)))
    w_up = bell_draw(streams_of[4], (EXPERTS * GROUP, D, FF // GROUP), D ** -0.5, 0.09375, ((0, 8), (2, 4)))
    w_down = bell_draw(streams_of[5], (EXPERTS * GROUP, FF // GROUP, D), FF ** -0.5, 0.0546875, ((0, 8), (1, 4)))
    states = bell_draw(streams_of[6], (N_DP * SLOTS, NST, CHANNELS), 1.0, 6.0, ((0, 8), (2, 4)))
    kv_blocks = bell_draw(streams_of[7], (N_DP * BLOCKS, 2, BLK, KVH * HEAD), 1.0, 6.0, ((0, 8), (3, 4)))
    plan_slots = draw_plan_slots(jax.random.fold_in(streams_of[11], 71), 0)
    plan_len = draw_plan_len(jax.random.fold_in(streams_of[11], 71), 0)
    plan_blocks = draw_plan_blocks(jax.random.fold_in(streams_of[11], 71), 0)
    return dict(tokens=tokens, router=router, expert_ids=expert_ids, w_gate=w_gate, w_up=w_up, w_down=w_down, states=states, kv_blocks=kv_blocks, plan_slots=plan_slots, plan_len=plan_len, plan_blocks=plan_blocks)


def reference(tokens, router, expert_ids, w_gate, w_up, w_down, states, kv_blocks, plan_slots, plan_len, plan_blocks):
    devices_all = N_DP * N_EP
    block_tokens = tokens.reshape(devices_all, TOK_DEV, D)
    pick_ids = expert_ids.reshape(devices_all, TOK_DEV * 2).astype(jnp.int32)
    onehot = (pick_ids[:, :, None] == jnp.arange(EXPERTS, dtype=jnp.int32)[None, None, :]).astype(jnp.int32)
    earlier = jnp.cumsum(onehot, axis=1) - onehot
    slot_of = jnp.sum(earlier * onehot, axis=2).astype(jnp.int32)
    target_row = (pick_ids * CAP + slot_of).astype(jnp.int32)
    doubled = jnp.repeat(block_tokens, 2, axis=1)
    device_line = jnp.broadcast_to(jnp.arange(devices_all, dtype=jnp.int32)[:, None], target_row.shape)
    packed = jnp.zeros((devices_all, EXPERTS * CAP, D), tokens.dtype)
    packed = packed.at[device_line.reshape(-1), target_row.reshape(-1)].set(doubled.reshape(-1, D))
    expert_rows = packed.reshape(devices_all, EXPERTS, CAP, D).transpose(1, 0, 2, 3).reshape(EXPERTS, devices_all * CAP, D)
    slab_width = FF // GROUP
    gate_all = w_gate.reshape(EXPERTS, GROUP, D, slab_width)
    up_all = w_up.reshape(EXPERTS, GROUP, D, slab_width)
    down_all = w_down.reshape(EXPERTS, GROUP * slab_width, D)

    def run_expert(operands):
        rows, gate_slabs, up_slabs, down_matrix = operands
        gate_matrix = gate_slabs.transpose(1, 0, 2).reshape(D, FF)
        up_matrix = up_slabs.transpose(1, 0, 2).reshape(D, FF)
        gate = jnp.dot(rows, gate_matrix, preferred_element_type=jnp.float32)
        upper = jnp.dot(rows, up_matrix, preferred_element_type=jnp.float32)
        hidden = (jax.nn.silu(gate) * upper).astype(jnp.bfloat16)
        return jnp.dot(hidden, down_matrix, preferred_element_type=jnp.float32)

    expert_out = lax.map(run_expert, (expert_rows, gate_all, up_all, down_all))
    expert_out = expert_out.reshape(EXPERTS, devices_all, CAP, D)
    chosen = expert_out[pick_ids, device_line, slot_of]
    chosen = chosen.reshape(TOKENS, 2, D)
    logits = jnp.dot(tokens.astype(jnp.float32), router, precision=lax.Precision.HIGHEST)
    scores = jax.nn.sigmoid(jnp.take_along_axis(logits, expert_ids.astype(jnp.int32), axis=1))
    weights = scores / jnp.sum(scores, axis=1, keepdims=True)
    mixed = jnp.sum(weights[:, :, None] * chosen, axis=1).astype(jnp.bfloat16)

    rank_line = jnp.arange(N_DP, dtype=jnp.int32)
    slot_states = states.reshape(N_DP, SLOTS, NST, CHANNELS)
    leaving_slot = plan_slots[:, :, 0].astype(jnp.int32)
    target_rank = plan_slots[:, :, 1].astype(jnp.int32)
    target_slot = plan_slots[:, :, 2].astype(jnp.int32)
    gone = jnp.any(leaving_slot[:, :, None] == jnp.arange(SLOTS, dtype=jnp.int32)[None, None, :], axis=1)
    payload = slot_states[rank_line[:, None], jnp.maximum(leaving_slot, 0)]
    payload = jnp.where((leaving_slot >= 0)[:, :, None, None], payload, jnp.zeros_like(payload))
    new_states = jnp.where(gone[:, :, None, None], jnp.zeros_like(slot_states), slot_states)
    rank_index = jnp.where(target_rank >= 0, target_rank, N_DP).astype(jnp.int32)
    slot_index = jnp.maximum(target_slot, 0).astype(jnp.int32)
    new_states = new_states.at[rank_index.reshape(-1), slot_index.reshape(-1)].set(payload.reshape(-1, NST, CHANNELS), mode="drop")
    new_states = new_states.reshape(N_DP * SLOTS, NST, CHANNELS)

    cache = kv_blocks.reshape(N_DP, BLOCKS, 2, BLK, KVH * HEAD)
    leaving_block = plan_blocks[:, :, 0, :].astype(jnp.int32)
    taken_block = plan_blocks[:, :, 1, :].astype(jnp.int32)
    gone_blocks = jnp.any(leaving_block.reshape(N_DP, -1)[:, :, None] == jnp.arange(BLOCKS, dtype=jnp.int32)[None, None, :], axis=1)
    cache_payload = cache[rank_line[:, None, None], jnp.maximum(leaving_block, 0)]
    position = jnp.arange(BPR, dtype=jnp.int32)[:, None] * BLK + jnp.arange(BLK, dtype=jnp.int32)[None, :]
    written = (leaving_block >= 0)[:, :, :, None] & (position[None, None] < plan_len.astype(jnp.int32)[:, :, None, None])
    cache_payload = jnp.where(written[:, :, :, None, :, None], cache_payload, jnp.zeros_like(cache_payload))
    new_cache = jnp.where(gone_blocks[:, :, None, None, None], jnp.zeros_like(cache), cache)
    block_rank = jnp.where(taken_block >= 0, jnp.broadcast_to(target_rank[:, :, None], taken_block.shape), N_DP).astype(jnp.int32)
    block_index = jnp.maximum(taken_block, 0).astype(jnp.int32)
    new_cache = new_cache.at[block_rank.reshape(-1), block_index.reshape(-1)].set(cache_payload.reshape(-1, 2, BLK, KVH * HEAD), mode="drop")
    new_cache = new_cache.reshape(N_DP * BLOCKS, 2, BLK, KVH * HEAD)
    return mixed, new_states, new_cache
```

```python
import functools

import jax
import jax.numpy as jnp
from jax import lax
from jax.experimental import pallas as pl
from jax.experimental.pallas import tpu as pltpu
from jax.sharding import PartitionSpec as P

CAP = 2
MESH = pl.DeviceIdType.MESH
ANY = pl.BlockSpec(memory_space=pl.ANY)
VMEM = pl.BlockSpec(memory_space=pltpu.VMEM)
SMEM = pl.BlockSpec(memory_space=pltpu.SMEM)
VMEM_LIMIT = 65_000_000
TILE = 256
RING = 13
EARLY = 2
LAND_LIMIT = 1 << 20


def target_rows(ids_ref, tok_count):
    picks = [ids_ref[k, t] for t in range(tok_count) for k in range(2)]
    rows = []
    for p, expert in enumerate(picks):
        slot = jnp.int32(0)
        for q in range(p):
            slot = slot + jnp.where(picks[q] == expert, 1, 0)
        rows.append(expert * CAP + slot)
    return picks, rows


def land_kernel(states_ref, cache_ref, mixed_ref, new_states, new_cache, new_mixed, sem):
    pairs = ((states_ref, new_states), (cache_ref, new_cache), (mixed_ref, new_mixed))
    copies = [pltpu.make_async_copy(a, b, sem.at[i]) for i, (a, b) in enumerate(pairs)]
    for copy in copies:
        copy.start()
    for copy in copies:
        copy.wait()


def expert_kernel(
    ranks, quads,
    ids_hbm, slots_hbm, len_hbm, blocks_hbm, tok_hbm, router_hbm, gate_ref, up_ref, down_ref,
    states_ref, kv_ref,
    new_states, new_cache, mixed_ref,
    ids_ref, slots_ref, len_ref, blocks_ref, tok_ref, router_ref,
    packed_ref, s_all, c_all, s_pay, c_pay, s_got, c_got,
    w_buf, x_in, x_all, hidden, keep, pair_send, pair_recv, send_buf, recv_buf,
    small_sem, big_sem, w_sem, first_send, first_recv, cross_send, cross_recv, pair_sems,
    half_send, half_recv, back_send, back_recv, mig_send, mig_recv,
):
    d = lax.axis_index("dp")
    e = lax.axis_index("ep")
    side, core = e // 2, lax.rem(e, 2)
    across, twin = (1 - side) * 2 + core, side * 2 + 1 - core
    experts = ranks
    up_tiles = gate_ref.shape[2] // TILE
    down_tiles = down_ref.shape[2] // (2 * TILE)
    depth = down_ref.shape[1]
    ring = w_buf.shape[0]
    rows_half = 2 * ranks * CAP
    owners = 2 * ranks
    me = side * ranks + d

    barrier = pltpu.get_barrier_semaphore()

    @pl.loop(1, owners)
    def _(k):
        other = lax.rem(me + k, owners)
        pl.semaphore_signal(
            barrier, inc=1, device_id=(lax.rem(other, ranks), (other // ranks) * 2 + core),
            device_id_type=MESH,
        )

    pl.semaphore_signal(barrier, inc=1, device_id=(d, twin), device_id_type=MESH)

    smalls = [
        pltpu.make_async_copy(a, b, small_sem.at[i])
        for i, (a, b) in enumerate((
            (tok_hbm, tok_ref), (ids_hbm, ids_ref), (router_hbm, router_ref),
            (slots_hbm, slots_ref), (len_hbm, len_ref), (blocks_hbm, blocks_ref),
        ))
    ]
    for copy in smalls:
        copy.start()

    def up_copies(j):
        columns = pl.ds(pl.multiple_of(j * TILE, TILE), TILE)
        return (
            pltpu.make_async_copy(gate_ref.at[0, :, columns], w_buf.at[j, 0], w_sem.at[j, 0]),
            pltpu.make_async_copy(up_ref.at[0, :, columns], w_buf.at[j, 1], w_sem.at[j, 1]),
        )

    def down_copies(c):
        slot = lax.rem(up_tiles + c, ring)
        found = []
        for h in range(2):
            columns = pl.ds(pl.multiple_of((2 * c + h) * TILE, TILE), TILE)
            found.append(pltpu.make_async_copy(
                down_ref.at[0, :, columns], w_buf.at[slot, h, pl.ds(0, depth)], w_sem.at[slot, h]
            ))
        return found

    load_states = pltpu.make_async_copy(states_ref, s_all, big_sem.at[0])
    load_cache = pltpu.make_async_copy(kv_ref, c_all, big_sem.at[1])

    @pl.loop(0, EARLY)
    def _(j):
        for copy in up_copies(j):
            copy.start()

    load_states.start()
    load_cache.start()

    @pl.loop(EARLY, up_tiles)
    def _(j):
        for copy in up_copies(j):
            copy.start()

    @pl.loop(0, ring - up_tiles)
    def _(c):
        for copy in down_copies(c):
            copy.start()

    smalls[0].wait()
    smalls[1].wait()
    tok_count = tok_ref.shape[0]
    picks, rows = target_rows(ids_ref, tok_count)
    row_at = lax.broadcasted_iota(jnp.int32, (experts * CAP, tok_count), 0)
    tok_at = lax.broadcasted_iota(jnp.int32, (experts * CAP, tok_count), 1)
    placer = jnp.zeros((experts * CAP, tok_count), jnp.float32)
    for p, row in enumerate(rows):
        placer = jnp.where((row_at == row) & (tok_at == p // 2), 1.0, placer)
    packed = jnp.dot(
        placer.astype(jnp.bfloat16), tok_ref[...], preferred_element_type=jnp.float32
    ).astype(jnp.bfloat16)
    for r in range(experts):
        packed_ref[r] = packed[r * CAP : (r + 1) * CAP]
    x_in[e, d] = packed_ref[d]

    pl.semaphore_wait(barrier, owners)

    for k in range(1, ranks):
        peer = lax.rem(d + k, ranks)
        pltpu.make_async_remote_copy(
            packed_ref.at[peer], x_in.at[e, d], first_send, first_recv.at[k],
            device_id=(peer, e), device_id_type=MESH,
        ).start()

    def cross(src, source, k):
        return pltpu.make_async_remote_copy(
            src, x_in.at[e, source], cross_send, cross_recv.at[k],
            device_id=(d, across), device_id_type=MESH,
        )

    def to_twin(src, quad, source):
        return pltpu.make_async_remote_copy(
            src, x_in.at[quad, source], pair_sems.at[0], pair_sems.at[1],
            device_id=(d, twin), device_id_type=MESH,
        )

    cross(packed_ref.at[d], d, 0).start()
    to_twin(packed_ref.at[d], e, d).start()

    smalls[2].wait()
    wide = tok_ref[...].astype(jnp.float32)
    lane = lax.broadcasted_iota(jnp.int32, (tok_count, experts), 1)
    seat = lax.broadcasted_iota(jnp.int32, (tok_count, experts), 0)
    logits = jnp.zeros((tok_count, experts), jnp.float32)
    for r in range(experts):
        product = jnp.sum(wide * router_ref[r : r + 1, :], axis=1, keepdims=True)
        logits = jnp.where(lane == r, product, logits)
    column = lax.broadcasted_iota(jnp.int32, (tok_count, owners * CAP), 1)
    token = lax.broadcasted_iota(jnp.int32, (tok_count, owners * CAP), 0)
    row_of = lax.rem(column, ranks * CAP)
    scores, hits = [], []
    for k in range(2):
        chosen = jnp.zeros(logits.shape, jnp.int32)
        target = jnp.zeros(column.shape, jnp.int32)
        for t in range(tok_count):
            chosen = jnp.where(seat == t, picks[2 * t + k], chosen)
            target = jnp.where(token == t, rows[2 * t + k], target)
        value = jnp.sum(jnp.where(lane == chosen, logits, 0.0), axis=1, keepdims=True)
        scores.append(jax.nn.sigmoid(value))
        hits.append(row_of == target)
    total = scores[0] + scores[1]
    comb = jnp.where(hits[0], scores[0] / total, 0.0) + jnp.where(hits[1], scores[1] / total, 0.0)
    comb_high = comb.astype(jnp.bfloat16)
    comb_low = (comb - comb_high.astype(jnp.float32)).astype(jnp.bfloat16)

    def source_of(k):
        return lax.rem(d - k + ranks, ranks)

    def relay(k):
        source = source_of(k)
        cross(x_in.at[across, source], source, k).wait_recv()
        to_twin(x_in.at[across, source], across, source).start()

    for k in range(1, ranks):
        source = source_of(k)
        pltpu.make_async_remote_copy(
            packed_ref.at[d], x_in.at[e, source], first_send, first_recv.at[k],
            device_id=(source, e), device_id_type=MESH,
        ).wait_recv()
        cross(x_in.at[e, source], source, k).start()
        to_twin(x_in.at[e, source], e, source).start()
        if k >= 2:
            relay(k - 2)

    relay(ranks - 2)
    relay(ranks - 1)

    for copy in smalls[3:]:
        copy.wait()
    load_states.wait()
    load_cache.wait()
    moves = slots_ref.shape[1]
    per_request = blocks_ref.shape[2]
    block_len = kv_ref.shape[2]
    position = lax.broadcasted_iota(jnp.int32, kv_ref.shape[1:], 1)
    for m in range(moves):
        s_pay[0, m] = s_all[jnp.maximum(slots_ref[0, m, d], 0)]
        for j in range(per_request):
            kept = c_all[jnp.maximum(blocks_ref[m, 0, j, d], 0)].astype(jnp.float32)
            kept = jnp.where(j * block_len + position < len_ref[m, d], kept, 0.0)
            c_pay[0, m, j] = kept.astype(jnp.bfloat16)
    shifts = []
    for m in range(moves):
        shift = jnp.int32(0)
        for r in range(ranks):
            gap = slots_ref[1, m, r] - r
            gap = gap + jnp.where(gap < 0, ranks, 0)
            shift = jnp.where(slots_ref[1, m, r] >= 0, gap, shift)
        shifts.append(shift)
    bits = ranks.bit_length() - 1

    def bit_of(m, step):
        return 0 if step == bits - 1 else bits - 1 - (step + m) % (bits - 1)

    def hop_copies(m, step):
        bit = 1 << bit_of(m, step)
        peer = d + bit - 2 * bit * lax.rem(d // bit, 2)
        return [
            pltpu.make_async_remote_copy(
                pay.at[step, m], got.at[step, m], mig_send.at[i, step, m], mig_recv.at[i, step, m],
                device_id=(peer, e), device_id_type=MESH,
            )
            for i, (pay, got) in enumerate(((s_pay, s_got), (c_pay, c_got)))
        ]

    def hop_start(step):
        for m in range(moves):
            for copy in hop_copies(m, step):
                copy.start()

    def hop_finish(step):
        for m in range(moves):
            for copy in hop_copies(m, step):
                copy.wait_recv()
            bit = 1 << bit_of(m, step)
            fixed = sum(1 << bit_of(m, s) for s in range(step + 1))
            loose = ranks - 1 - fixed
            swap = jnp.int32(0)
            for r in range(ranks):
                reach = (r + shifts[m]) & (ranks - 1)
                held = (((d ^ r) & loose) | ((d ^ reach) & fixed)) == 0
                swap = jnp.where(held & (((d ^ r) & bit) != 0), 1, swap)
            swap = swap > 0
            s_pay[step + 1, m] = lax.select(swap, s_got[step, m], s_pay[step, m])
            c_pay[step + 1, m] = lax.select(swap, c_got[step, m], c_pay[step, m])

    hop_start(0)

    def gather(which):
        for half in range(2):
            at = pl.multiple_of((which * 2 + half) * ranks * CAP, ranks * CAP)
            x_all[pl.ds(at, ranks * CAP), :] = jnp.concatenate(
                [x_in[half * 2 + which, r] for r in range(ranks)], axis=0
            )

    gather(core)
    arrivals = x_in.at[pl.ds(0, 2)]
    pltpu.make_async_copy(arrivals, arrivals, pair_sems.at[1]).wait()
    gather(1 - core)

    def up_step(j):
        for copy in up_copies(j):
            copy.wait()
        gate = jnp.dot(x_all[...], w_buf[j, 0], preferred_element_type=jnp.float32)
        upper = jnp.dot(x_all[...], w_buf[j, 1], preferred_element_type=jnp.float32)
        value = gate / (1.0 + jnp.exp(-gate)) * upper
        hidden[:, pl.ds(pl.multiple_of(j * TILE, TILE), TILE)] = value.astype(jnp.bfloat16)
        later = j + ring - up_tiles

        @pl.when(later < down_tiles)
        def _():
            for copy in down_copies(later):
                copy.start()

    for part in range(2):
        pl.loop(part * up_tiles // 2, (part + 1) * up_tiles // 2)(up_step)
        if part + 1 < bits:
            hop_finish(part)
            hop_start(part + 1)

    def swap_copy(c):
        return pltpu.make_async_remote_copy(
            pair_send.at[c], pair_recv.at[c], half_send.at[c], half_recv.at[c],
            device_id=(d, twin), device_id_type=MESH,
        )

    def send_home(c):
        swap_copy(c).wait_recv()
        whole = (keep[c] + pair_recv[c]).astype(jnp.bfloat16)
        for o in range(owners):
            send_buf[c, o] = whole[o * CAP : (o + 1) * CAP]
        recv_buf[c, me] = send_buf[c, me]

        @pl.loop(1, owners)
        def _(k):
            other = lax.rem(me + k, owners)
            pltpu.make_async_remote_copy(
                send_buf.at[c, other], recv_buf.at[c, me], back_send.at[c], back_recv.at[c],
                device_id=(lax.rem(other, ranks), (other // ranks) * 2 + core), device_id_type=MESH,
            ).start()

    @pl.loop(0, down_tiles)
    def _(c):
        slot = lax.rem(up_tiles + c, ring)
        for copy in down_copies(c):
            copy.wait()
        for h in range(2):
            part = jnp.dot(
                hidden[...], w_buf[slot, h, pl.ds(0, depth)], preferred_element_type=jnp.float32
            )
            low, high = part[:rows_half], part[rows_half:]
            first = core == 0
            columns = pl.ds(h * TILE, TILE)
            keep[c, :, columns] = lax.select(first, low, high)
            pair_send[c, :, columns] = lax.select(first, high, low)
        swap_copy(c).start()

        @pl.when(c > 0)
        def _():
            send_home(c - 1)

    send_home(down_tiles - 1)
    hop_finish(bits - 1)

    leaving, landing = [], []
    for m in range(moves):
        anchor, arriving = jnp.int32(0), jnp.int32(0)
        for r in range(ranks):
            hit = slots_ref[1, m, r] == d
            anchor = jnp.where(hit, r, anchor)
            arriving = jnp.where(hit, 1, arriving)
        leaving.append((slots_ref[0, m, d], [blocks_ref[m, 0, j, d] for j in range(per_request)]))
        landing.append((
            jnp.where(arriving > 0, slots_ref[2, m, anchor], -1),
            [jnp.where(arriving > 0, blocks_ref[m, 1, j, anchor], -1) for j in range(per_request)],
        ))

    @pl.loop(0, s_all.shape[0])
    def _(s):
        value = s_all[s]
        for m in range(moves):
            value = lax.select(leaving[m][0] == s, jnp.zeros_like(value), value)
        for m in range(moves):
            value = lax.select(landing[m][0] == s, s_pay[bits, m], value)
        new_states[s] = value

    @pl.loop(0, c_all.shape[0])
    def _(s):
        value = c_all[s]
        for m in range(moves):
            for j in range(per_request):
                value = lax.select(leaving[m][1][j] == s, jnp.zeros_like(value), value)
        for m in range(moves):
            for j in range(per_request):
                value = lax.select(landing[m][1][j] == s, c_pay[bits, m, j], value)
        new_cache[s] = value

    @pl.loop(0, down_tiles)
    def _(c):
        most = recv_buf.at[c, pl.ds(0, owners - 1)]
        pltpu.make_async_copy(most, most, back_recv.at[c]).wait()
        rows_in = jnp.concatenate([recv_buf[c, o] for o in range(owners)], axis=0)
        high = jnp.dot(comb_high, rows_in, preferred_element_type=jnp.float32)
        low = jnp.dot(comb_low, rows_in, preferred_element_type=jnp.float32)
        mixed_ref[:, pl.ds(pl.multiple_of(c * 2 * TILE, 2 * TILE), 2 * TILE)] = (
            high + low
        ).astype(jnp.bfloat16)

    for step in range(bits):
        for m in range(moves):
            for copy in hop_copies(m, step):
                copy.wait_send()
    most = packed_ref.at[pl.ds(0, ranks - 1)]
    pltpu.make_async_copy(most, most, first_send).wait()
    most = x_in.at[0]
    pltpu.make_async_copy(most, most, cross_send).wait()
    pltpu.make_async_copy(arrivals, arrivals, pair_sems.at[0]).wait()

    @pl.loop(0, down_tiles)
    def _(c):
        swap_copy(c).wait_send()
        most = send_buf.at[c, pl.ds(0, owners - 1)]
        pltpu.make_async_copy(most, most, back_send.at[c]).wait()


def fused(
    tokens, router, expert_ids, w_gate, w_up, w_down, states, kv_blocks,
    plan_slots, plan_len, plan_blocks,
):
    ranks, quads = lax.axis_size("dp"), lax.axis_size("ep")
    experts = router.shape[1]
    tok_count, width = tokens.shape
    moves = plan_slots.shape[1]
    per_request = plan_blocks.shape[3]
    bf16 = jnp.bfloat16
    dma = pltpu.SemaphoreType.DMA
    like = jax.ShapeDtypeStruct
    state_one, cache_one = states.shape[1:], kv_blocks.shape[1:]
    ids = expert_ids.T
    slots = jnp.transpose(plan_slots, (2, 1, 0))
    lengths = plan_len.T
    blocks = jnp.transpose(plan_blocks, (1, 2, 3, 0))
    routes = router.T
    depth = w_gate.shape[2]
    down_tiles = width // (2 * TILE)
    owners = 2 * ranks
    bits = ranks.bit_length() - 1
    outputs = pl.pallas_call(
        functools.partial(expert_kernel, ranks, quads),
        out_shape=(
            pltpu.VMEM(states.shape, bf16),
            pltpu.VMEM(kv_blocks.shape, bf16),
            pltpu.VMEM(tokens.shape, bf16),
        ),
        in_specs=[ANY] * 11,
        out_specs=(VMEM, VMEM, VMEM),
        scratch_shapes=[
            pltpu.SMEM(ids.shape, jnp.int32),
            pltpu.SMEM(slots.shape, jnp.int32),
            pltpu.SMEM(lengths.shape, jnp.int32),
            pltpu.SMEM(blocks.shape, jnp.int32),
            pltpu.VMEM(tokens.shape, bf16),
            pltpu.VMEM(routes.shape, jnp.float32),
            pltpu.VMEM((experts, CAP, width), bf16),
            pltpu.VMEM(states.shape, bf16),
            pltpu.VMEM(kv_blocks.shape, bf16),
            pltpu.VMEM((bits + 1, moves, *state_one), bf16),
            pltpu.VMEM((bits + 1, moves, per_request, *cache_one), bf16),
            pltpu.VMEM((bits, moves, *state_one), bf16),
            pltpu.VMEM((bits, moves, per_request, *cache_one), bf16),
            pltpu.VMEM((RING, 2, width, TILE), bf16),
            pltpu.VMEM((quads, ranks, CAP, width), bf16),
            pltpu.VMEM((quads * ranks * CAP, width), bf16),
            pltpu.VMEM((quads * ranks * CAP, depth), bf16),
            pltpu.VMEM((down_tiles, owners * CAP, 2 * TILE), jnp.float32),
            pltpu.VMEM((down_tiles, owners * CAP, 2 * TILE), jnp.float32),
            pltpu.VMEM((down_tiles, owners * CAP, 2 * TILE), jnp.float32),
            pltpu.VMEM((down_tiles, owners, CAP, 2 * TILE), bf16),
            pltpu.VMEM((down_tiles, owners, CAP, 2 * TILE), bf16),
            dma((6,)), dma((2,)), dma((RING, 2)), dma, dma((ranks,)), dma, dma((ranks,)), dma((2,)),
            dma((down_tiles,)), dma((down_tiles,)), dma((down_tiles,)), dma((down_tiles,)),
            dma((2, bits, moves)), dma((2, bits, moves)),
        ],
        compiler_params=pltpu.CompilerParams(
            collective_id=0, has_side_effects=True, vmem_limit_bytes=VMEM_LIMIT
        ),
        name="expert",
    )(
        ids, slots, lengths, blocks, tokens, routes, w_gate, w_up, w_down, states, kv_blocks
    )
    outputs = [pltpu.with_memory_space_constraint(o, pltpu.VMEM) for o in outputs]
    new_states, new_cache, mixed = pl.pallas_call(
        land_kernel,
        out_shape=(like(states.shape, bf16), like(kv_blocks.shape, bf16), like(tokens.shape, bf16)),
        in_specs=[VMEM] * 3,
        out_specs=(ANY, ANY, ANY),
        scratch_shapes=[dma((3,))],
        compiler_params=pltpu.CompilerParams(vmem_limit_bytes=LAND_LIMIT),
        name="land",
    )(*outputs)
    return mixed, new_states, new_cache


def local(
    tokens,
    router,
    expert_ids,
    w_gate,
    w_up,
    w_down,
    states,
    kv_blocks,
    plan_slots,
    plan_len,
    plan_blocks,
):
    ranks = lax.axis_size("dp")
    here = lax.axis_index("dp")
    moves = plan_slots.shape[1]
    slot_count = states.shape[0]
    block_count = kv_blocks.shape[0]
    per_request = plan_blocks.shape[3]
    block_len = kv_blocks.shape[2]
    mine = lax.dynamic_index_in_dim(plan_slots, here, 0, keepdims=False)
    my_blocks = lax.dynamic_index_in_dim(plan_blocks, here, 0, keepdims=False)
    my_length = lax.dynamic_index_in_dim(plan_len, here, 0, keepdims=False)
    leaving_slot = mine[:, 0]
    leaving_block = my_blocks[:, 0, :]
    state_out = states[jnp.maximum(leaving_slot, 0)]
    state_out = jnp.where((leaving_slot >= 0)[:, None, None], state_out, jnp.zeros_like(state_out))
    cache_out = kv_blocks[jnp.maximum(leaving_block, 0)]
    position = jnp.arange(per_request)[:, None] * block_len + jnp.arange(block_len)[None, :]
    written = (leaving_block >= 0)[:, :, None] & (position[None] < my_length[:, None, None])
    cache_out = jnp.where(written[:, :, None, :, None], cache_out, jnp.zeros_like(cache_out))
    arrivals = plan_slots[:, :, 1] == here
    sender = jnp.sum(jnp.where(arrivals, jnp.arange(ranks)[:, None], 0), axis=0)
    arriving = jnp.any(arrivals, axis=0)
    peers = jnp.arange(ranks)
    match = mine[:, 1][None, :] == peers[:, None]
    which = jnp.sum(jnp.where(match, jnp.arange(moves)[None, :], 0), axis=1)
    filled = jnp.any(match, axis=1)
    send_state = jnp.where(
        filled[:, None, None], state_out[which], jnp.zeros_like(state_out[which])
    )
    send_cache = jnp.where(
        filled[:, None, None, None, None], cache_out[which], jnp.zeros_like(cache_out[which])
    )
    got_state, got_cache = (
        lax.all_to_all(send_state, "dp", split_axis=0, concat_axis=0, tiled=True),
        lax.all_to_all(send_cache, "dp", split_axis=0, concat_axis=0, tiled=True),
    )
    state_in = got_state[sender]
    cache_in = got_cache[sender]
    slot_line = jnp.arange(slot_count)
    gone = jnp.any(slot_line[:, None] == leaving_slot[None, :], axis=1)
    new_states = jnp.where(gone[:, None, None], jnp.zeros_like(states), states)
    block_line = jnp.arange(block_count)
    gone_blocks = jnp.any(block_line[:, None, None] == leaving_block[None], axis=(1, 2))
    new_cache = jnp.where(gone_blocks[:, None, None, None], jnp.zeros_like(kv_blocks), kv_blocks)
    for move_index in range(moves):
        anchor = sender[move_index]
        place = plan_slots[anchor, move_index, 2]
        landing = (slot_line == place) & arriving[move_index]
        new_states = jnp.where(landing[:, None, None], state_in[move_index][None], new_states)
        for block_index in range(per_request):
            spot = plan_blocks[anchor, move_index, 1, block_index]
            block_hit = (block_line == spot) & arriving[move_index]
            new_cache = jnp.where(
                block_hit[:, None, None, None], cache_in[move_index, block_index][None], new_cache
            )
    experts = router.shape[1]
    tok_count = tokens.shape[0]
    width = tokens.shape[1]
    group = ranks // experts
    flat_ids = expert_ids.reshape(-1)
    onehot = (flat_ids[:, None] == jnp.arange(experts)[None, :]).astype(jnp.int32)
    earlier = jnp.cumsum(onehot, axis=0) - onehot
    slot_of = jnp.sum(earlier * onehot, axis=1)
    target_row = flat_ids * CAP + slot_of
    placer = (jnp.arange(experts * CAP)[:, None] == target_row[None, :]).astype(jnp.bfloat16)
    doubled = jnp.repeat(tokens, 2, axis=0)
    packed = jnp.dot(placer, doubled, preferred_element_type=jnp.float32).astype(jnp.bfloat16)
    outgoing = jnp.repeat(packed.reshape(experts, CAP, width), group, axis=0)
    incoming = lax.all_to_all(outgoing, "dp", split_axis=0, concat_axis=0, tiled=True)
    rows_in = incoming.reshape(ranks * CAP, width)
    piece = lax.all_gather(rows_in, "ep", axis=0, tiled=True)
    gate = jnp.dot(piece, w_gate[0], preferred_element_type=jnp.float32)
    upper = jnp.dot(piece, w_up[0], preferred_element_type=jnp.float32)
    hidden = (jax.nn.silu(gate) * upper).astype(jnp.bfloat16)
    summed = lax.psum_scatter(
        jnp.dot(hidden, w_down[0], preferred_element_type=jnp.float32),
        "ep",
        scatter_dimension=0,
        tiled=True,
    )
    returned = lax.all_to_all(
        summed.reshape(ranks, CAP, width), "dp", split_axis=0, concat_axis=0, tiled=True
    )
    expert_out = jnp.sum(returned.reshape(experts, group, CAP, width), axis=1).reshape(
        experts * CAP, width
    )
    chosen = expert_out[target_row].reshape(tok_count, 2, width)
    logits = jnp.dot(tokens.astype(jnp.float32), router, precision=lax.Precision.HIGHEST)
    scores = jax.nn.sigmoid(jnp.take_along_axis(logits, expert_ids, axis=1))
    weights = scores / jnp.sum(scores, axis=1, keepdims=True)
    mixed = jnp.sum(weights[:, :, None] * chosen, axis=1).astype(jnp.bfloat16)
    return (mixed, new_states, new_cache)


def solution(mesh):
    placed = (
        P(("dp", "ep"), None),
        P(),
        P(("dp", "ep"), None),
        P("dp", None, "ep"),
        P("dp", None, "ep"),
        P("dp", "ep", None),
        P("dp", None, "ep"),
        P("dp", None, None, "ep"),
        P(),
        P(),
        P(),
    )
    def step(*args):
        ranks, quads = lax.axis_size("dp"), lax.axis_size("ep")
        one_slab = args[1].shape[1] == ranks and ranks & (ranks - 1) == 0
        two_by_two = quads == 2 * 2
        return (fused if one_slab and two_by_two else local)(*args)

    return jax.shard_map(
        step,
        mesh=mesh,
        in_specs=placed,
        out_specs=(P(("dp", "ep"), None), P("dp", None, "ep"), P("dp", None, None, "ep")),
        check_vma=False,
    )
```

```python
import functools

import jax
import jax.numpy as jnp
from jax import lax
from jax.experimental import pallas as pl
from jax.experimental.pallas import tpu as pltpu
from jax.sharding import PartitionSpec as P

CAP = 2
MESH = pl.DeviceIdType.MESH
ANY = pl.BlockSpec(memory_space=pl.ANY)
VMEM = pl.BlockSpec(memory_space=pltpu.VMEM)
SMEM = pl.BlockSpec(memory_space=pltpu.SMEM)
VMEM_LIMIT = 65_000_000
TILE = 256
RING = 13
EARLY = 2
WIDE = 2
PARTS = 2
SPLIT = 3
LAND_LIMIT = 1 << 20


def target_rows(ids_ref, tok_count):
    picks = [ids_ref[k, t] for t in range(tok_count) for k in range(2)]
    rows = []
    for p, expert in enumerate(picks):
        slot = jnp.int32(0)
        for q in range(p):
            slot = slot + jnp.where(picks[q] == expert, 1, 0)
        rows.append(expert * CAP + slot)
    return picks, rows


def land_kernel(states_ref, cache_ref, mixed_ref, new_states, new_cache, new_mixed, sem):
    pairs = ((states_ref, new_states), (cache_ref, new_cache), (mixed_ref, new_mixed))
    copies = [pltpu.make_async_copy(a, b, sem.at[i]) for i, (a, b) in enumerate(pairs)]
    for copy in copies:
        copy.start()
    for copy in copies:
        copy.wait()


def expert_kernel(
    ranks, quads,
    ids_hbm, slots_hbm, len_hbm, blocks_hbm, tok_hbm, router_hbm, gate_ref, up_ref, down_ref,
    states_ref, kv_ref,
    new_states, new_cache, mixed_ref,
    ids_ref, slots_ref, len_ref, blocks_ref, tok_ref, router_ref,
    packed_ref, s_all, c_all, pay, got,
    w_buf, x_in, x_all, part_sum, hidden, wide_keep, wide_pair, wide_home, slim_keep, slim_pair, slim_home,
    small_sem, big_sem, w_sem, first_send, first_recv, cross_send, cross_recv, pair_send, pair_recv,
    half_send, half_recv, back_send, back_recv, mig_send, mig_recv,
):
    d = lax.axis_index("dp")
    e = lax.axis_index("ep")
    side, core = e // 2, lax.rem(e, 2)
    across, twin = (1 - side) * 2 + core, side * 2 + 1 - core
    diagonal = (1 - side) * 2 + 1 - core
    experts = ranks
    up_tiles = gate_ref.shape[2] // TILE
    down_tiles = down_ref.shape[2] // (2 * TILE)
    depth = down_ref.shape[1]
    ring = w_buf.shape[0]
    rows_half = 2 * ranks * CAP
    owners = 2 * ranks
    span = packed_ref.shape[3]
    me = side * ranks + d

    barrier = pltpu.get_barrier_semaphore()

    @pl.loop(1, owners)
    def _(k):
        other = lax.rem(me + k, owners)
        pl.semaphore_signal(
            barrier, inc=1, device_id=(lax.rem(other, ranks), (other // ranks) * 2 + core),
            device_id_type=MESH,
        )

    for quad in (twin, diagonal):
        pl.semaphore_signal(barrier, inc=1, device_id=(d, quad), device_id_type=MESH)

    smalls = [
        pltpu.make_async_copy(a, b, small_sem.at[i])
        for i, (a, b) in enumerate((
            (tok_hbm, tok_ref), (ids_hbm, ids_ref), (router_hbm, router_ref),
            (slots_hbm, slots_ref), (len_hbm, len_ref), (blocks_hbm, blocks_ref),
        ))
    ]
    for copy in smalls:
        copy.start()

    def up_copies(j):
        columns = pl.ds(pl.multiple_of(j * TILE, TILE), TILE)
        return (
            pltpu.make_async_copy(gate_ref.at[0, :, columns], w_buf.at[j, 0], w_sem.at[j]),
            pltpu.make_async_copy(up_ref.at[0, :, columns], w_buf.at[j, 1], w_sem.at[j]),
        )

    def up_wait(j):
        pltpu.make_async_copy(w_buf.at[j], w_buf.at[j], w_sem.at[j]).wait()

    def down_copies(c):
        slot = lax.rem(up_tiles + c, ring)
        found = []
        for h in range(2):
            columns = pl.ds(pl.multiple_of((2 * c + h) * TILE, TILE), TILE)
            found.append(pltpu.make_async_copy(
                down_ref.at[0, :, columns], w_buf.at[slot, h, pl.ds(0, depth)], w_sem.at[slot]
            ))
        return found

    def down_wait(c):
        slot = lax.rem(up_tiles + c, ring)
        both = w_buf.at[slot, :, pl.ds(0, depth)]
        pltpu.make_async_copy(both, both, w_sem.at[slot]).wait()

    load_states = pltpu.make_async_copy(states_ref, s_all, big_sem.at[0])
    load_cache = pltpu.make_async_copy(kv_ref, c_all, big_sem.at[1])

    @pl.loop(0, EARLY)
    def _(j):
        for copy in up_copies(j):
            copy.start()

    load_states.start()
    load_cache.start()

    @pl.loop(EARLY, up_tiles)
    def _(j):
        for copy in up_copies(j):
            copy.start()

    @pl.loop(0, ring - up_tiles)
    def _(c):
        for copy in down_copies(c):
            copy.start()

    smalls[0].wait()
    smalls[1].wait()
    tok_count = tok_ref.shape[0]
    picks, rows = target_rows(ids_ref, tok_count)
    row_at = lax.broadcasted_iota(jnp.int32, (experts * CAP, tok_count), 0)
    tok_at = lax.broadcasted_iota(jnp.int32, (experts * CAP, tok_count), 1)
    placer = jnp.zeros((experts * CAP, tok_count), jnp.float32)
    for p, row in enumerate(rows):
        placer = jnp.where((row_at == row) & (tok_at == p // 2), 1.0, placer)
    packed = jnp.dot(
        placer.astype(jnp.bfloat16), tok_ref[...], preferred_element_type=jnp.float32
    ).astype(jnp.bfloat16)
    for h in range(PARTS):
        for r in range(experts):
            packed_ref[h, r] = packed[r * CAP : (r + 1) * CAP, h * span : (h + 1) * span]
        x_in[h, e, d] = packed_ref[h, d]

    pl.semaphore_wait(barrier, owners + 1)

    z_count = ranks // 2

    def planes(i, reverse):
        forward = (d // 2 < z_count // 2) == (not reverse)
        return jnp.where(forward, i, z_count - 1 - i)

    def cross(src, h, source):
        return pltpu.make_async_remote_copy(
            src, x_in.at[h, e, source], cross_send, cross_recv.at[h, source],
            device_id=(d, across), device_id_type=MESH,
        )

    def to_other(src, h, quad, source, where):
        return pltpu.make_async_remote_copy(
            src, x_in.at[h, quad, source], pair_send, pair_recv.at[h],
            device_id=(d, where), device_id_type=MESH,
        )

    def spread(src, h, source):
        cross(src, h, source).start()
        to_other(src, h, e, source, twin).start()

        @pl.when(core == 0)
        def _():
            to_other(src, h, e, source, diagonal).start()

    for h in range(PARTS):
        for i in range(z_count):
            plane = planes(i, True)
            for y in range(2):
                peer = plane * 2 + y

                @pl.when(peer != d)
                def _():
                    pltpu.make_async_remote_copy(
                        packed_ref.at[h, peer], x_in.at[h, e, d], first_send, first_recv.at[h, d],
                        device_id=(peer, e), device_id_type=MESH,
                    ).start()

        spread(packed_ref.at[h, d], h, d)

    smalls[2].wait()
    wide = tok_ref[...].astype(jnp.float32)
    lane = lax.broadcasted_iota(jnp.int32, (tok_count, experts), 1)
    seat = lax.broadcasted_iota(jnp.int32, (tok_count, experts), 0)
    logits = jnp.zeros((tok_count, experts), jnp.float32)
    for r in range(experts):
        product = jnp.sum(wide * router_ref[r : r + 1, :], axis=1, keepdims=True)
        logits = jnp.where(lane == r, product, logits)
    column = lax.broadcasted_iota(jnp.int32, (tok_count, owners * CAP), 1)
    token = lax.broadcasted_iota(jnp.int32, (tok_count, owners * CAP), 0)
    row_of = lax.rem(column, ranks * CAP)
    scores, hits = [], []
    for k in range(2):
        chosen = jnp.zeros(logits.shape, jnp.int32)
        target = jnp.zeros(column.shape, jnp.int32)
        for t in range(tok_count):
            chosen = jnp.where(seat == t, picks[2 * t + k], chosen)
            target = jnp.where(token == t, rows[2 * t + k], target)
        value = jnp.sum(jnp.where(lane == chosen, logits, 0.0), axis=1, keepdims=True)
        scores.append(jax.nn.sigmoid(value))
        hits.append(row_of == target)
    total = scores[0] + scores[1]
    comb = jnp.where(hits[0], scores[0] / total, 0.0) + jnp.where(hits[1], scores[1] / total, 0.0)
    comb_high = comb.astype(jnp.bfloat16)
    comb_low = (comb - comb_high.astype(jnp.float32)).astype(jnp.bfloat16)

    near = [planes(i, False) * 2 + y for i in range(z_count) for y in range(2)]

    def relay(h):
        for source in near:
            cross(x_in.at[h, across, source], h, source).wait_recv()

            @pl.when(core == 1)
            def _():
                to_other(x_in.at[h, across, source], h, across, source, twin).start()

    for h in range(PARTS):
        for source in near:

            @pl.when(source != d)
            def _():
                pltpu.make_async_remote_copy(
                    packed_ref.at[h, d], x_in.at[h, e, source], first_send, first_recv.at[h, source],
                    device_id=(source, e), device_id_type=MESH,
                ).wait_recv()
                spread(x_in.at[h, e, source], h, source)

    for copy in smalls[3:]:
        copy.wait()
    load_states.wait()
    load_cache.wait()
    moves = slots_ref.shape[1]
    per_request = blocks_ref.shape[2]
    block_len, lanes = kv_ref.shape[2:]
    pieces = states_ref.shape[2] // lanes
    position = lax.broadcasted_iota(jnp.int32, kv_ref.shape[1:], 1)
    for m in range(moves):
        state = s_all[jnp.maximum(slots_ref[0, m, d], 0)]
        for i in range(pieces):
            pay[0, m, i] = state[:, i * lanes : (i + 1) * lanes]
        for j in range(per_request):
            kept = c_all[jnp.maximum(blocks_ref[m, 0, j, d], 0)].astype(jnp.float32)
            kept = jnp.where(j * block_len + position < len_ref[m, d], kept, 0.0)
            pay[0, m, pl.ds(pieces + 2 * j, 2)] = kept.astype(jnp.bfloat16)
    shifts = []
    for m in range(moves):
        shift = jnp.int32(0)
        for r in range(ranks):
            gap = slots_ref[1, m, r] - r
            gap = gap + jnp.where(gap < 0, ranks, 0)
            shift = jnp.where(slots_ref[1, m, r] >= 0, gap, shift)
        shifts.append(shift)
    bits = ranks.bit_length() - 1

    def bit_of(m, step):
        return 0 if step == bits - 1 else bits - 1 - (step + m) % (bits - 1)

    def hop_copy(m, step):
        bit = 1 << bit_of(m, step)
        peer = d + bit - 2 * bit * lax.rem(d // bit, 2)
        return pltpu.make_async_remote_copy(
            pay.at[step, m], got.at[step, m], mig_send, mig_recv.at[step],
            device_id=(peer, e), device_id_type=MESH,
        )

    def hop_start(step):
        for m in range(moves):
            hop_copy(m, step).start()

    def hop_finish(step):
        pltpu.make_async_copy(got.at[step], got.at[step], mig_recv.at[step]).wait()
        for m in range(moves):
            bit = 1 << bit_of(m, step)
            fixed = sum(1 << bit_of(m, s) for s in range(step + 1))
            loose = ranks - 1 - fixed
            swap = jnp.int32(0)
            for r in range(ranks):
                reach = (r + shifts[m]) & (ranks - 1)
                held = (((d ^ r) & loose) | ((d ^ reach) & fixed)) == 0
                swap = jnp.where(held & (((d ^ r) & bit) != 0), 1, swap)
            pay[step + 1, m] = lax.select(swap > 0, got[step, m], pay[step, m])

    hop_start(0)
    relay(0)

    def gather(h, which):
        for half in range(2):
            at = pl.multiple_of((which * 2 + half) * ranks * CAP, ranks * CAP)
            x_all[pl.ds(at, ranks * CAP), h * span : (h + 1) * span] = jnp.concatenate(
                [x_in[h, half * 2 + which, r] for r in range(ranks)], axis=0
            )

    def pair_wait(h):
        most = x_in.at[h, pl.ds(0, 2)]
        pltpu.make_async_copy(most, most, pair_recv.at[h]).wait()

    gather(0, core)
    pair_wait(0)
    gather(0, 1 - core)

    def product(j, which, h):
        rows_of = pl.ds(h * span, span)
        return jnp.dot(x_all[:, rows_of], w_buf[j, which, rows_of], preferred_element_type=jnp.float32)

    def finish_up(j, gate, upper):
        value = gate / (1.0 + jnp.exp(-gate)) * upper
        hidden[:, pl.ds(pl.multiple_of(j * TILE, TILE), TILE)] = value.astype(jnp.bfloat16)

    def refill(j):
        later = j + ring - up_tiles

        @pl.when(later < down_tiles)
        def _():
            for copy in down_copies(later):
                copy.start()

    def tiles_of(i):
        return [i * WIDE + n for n in range(WIDE)]

    def first_step(i):
        for j in tiles_of(i):
            up_wait(j)
        for j in tiles_of(i):
            for which in range(2):
                part_sum[j, which] = product(j, which, 0)

    def second_step(i):
        for j in tiles_of(i):
            sums = [part_sum[j, which] for which in range(2)]
            for h in range(1, PARTS):
                sums = [sums[which] + product(j, which, h) for which in range(2)]
            finish_up(j, *sums)
        for j in tiles_of(i):
            refill(j)

    def whole_step(i):
        for j in tiles_of(i):
            up_wait(j)
        for j in tiles_of(i):
            gate, upper = [
                jnp.dot(x_all[...], w_buf[j, which], preferred_element_type=jnp.float32)
                for which in range(2)
            ]
            finish_up(j, gate, upper)
        for j in tiles_of(i):
            refill(j)

    split = part_sum.shape[0] // WIDE
    pl.loop(0, split - 1)(first_step)
    for h in range(1, PARTS):
        relay(h)
        gather(h, core)
    pl.loop(split - 1, split)(first_step)
    for h in range(1, PARTS):
        pair_wait(h)
        gather(h, 1 - core)
    hop_finish(0)
    hop_start(1)
    pl.loop(0, split)(second_step)
    pl.loop(split, up_tiles // WIDE)(whole_step)
    for step in range(1, bits - 1):
        hop_finish(step)
        hop_start(step + 1)

    wide_count = wide_keep.shape[0]
    groups = [(0, g, 2 * g, 2) for g in range(wide_count)]
    groups += [(1, g, 2 * wide_count + g, 1) for g in range(slim_keep.shape[0])]
    stores = ((wide_keep, wide_pair, wide_home), (slim_keep, slim_pair, slim_home))

    def swap_copy(n):
        kind, g, _, _ = groups[n]
        pair = stores[kind][1]
        return pltpu.make_async_remote_copy(
            pair.at[0, g], pair.at[1, g], half_send, half_recv.at[n],
            device_id=(d, twin), device_id_type=MESH,
        )

    def send_home(n):
        kind, g, _, _ = groups[n]
        keep, pair, home = stores[kind]
        swap_copy(n).wait_recv()
        whole = (keep[g] + pair[1, g]).astype(jnp.bfloat16)
        for o in range(owners):
            home[0, g, o] = whole[o * CAP : (o + 1) * CAP]
        home[1, g, me] = home[0, g, me]

        @pl.loop(1, owners, unroll=True)
        def _(k):
            other = lax.rem(me + k, owners)
            pltpu.make_async_remote_copy(
                home.at[0, g, other], home.at[1, g, me], back_send, back_recv.at[n],
                device_id=(lax.rem(other, ranks), (other // ranks) * 2 + core), device_id_type=MESH,
            ).start()

    def multiply(n):
        kind, g, start, count = groups[n]
        keep, pair, _ = stores[kind]
        for c in range(start, start + count):
            down_wait(c)
        for c in range(start, start + count):
            slot = lax.rem(up_tiles + c, ring)
            for h in range(2):
                part = jnp.dot(
                    hidden[...], w_buf[slot, h, pl.ds(0, depth)], preferred_element_type=jnp.float32
                )
                low, high = part[:rows_half], part[rows_half:]
                first = core == 0
                columns = pl.ds((2 * (c - start) + h) * TILE, TILE)
                keep[g, :, columns] = lax.select(first, low, high)
                pair[0, g, :, columns] = lax.select(first, high, low)
        swap_copy(n).start()

    def mix(n):
        kind, g, start, count = groups[n]
        home = stores[kind][2]
        most = home.at[1, g, pl.ds(0, owners - 1)]
        pltpu.make_async_copy(most, most, back_recv.at[n]).wait()
        rows_in = jnp.concatenate([home[1, g, o] for o in range(owners)], axis=0)
        high = jnp.dot(comb_high, rows_in, preferred_element_type=jnp.float32)
        low = jnp.dot(comb_low, rows_in, preferred_element_type=jnp.float32)
        mixed_ref[:, start * 2 * TILE : (start + count) * 2 * TILE] = (high + low).astype(jnp.bfloat16)

    for n in range(len(groups)):
        multiply(n)
        if n > 0:
            send_home(n - 1)
    send_home(len(groups) - 1)
    early = max(len(groups) - 2, 0)
    for n in range(early):
        mix(n)
    hop_finish(bits - 1)

    leaving, landing = [], []
    for m in range(moves):
        anchor, arriving = jnp.int32(0), jnp.int32(0)
        for r in range(ranks):
            hit = slots_ref[1, m, r] == d
            anchor = jnp.where(hit, r, anchor)
            arriving = jnp.where(hit, 1, arriving)
        leaving.append((slots_ref[0, m, d], [blocks_ref[m, 0, j, d] for j in range(per_request)]))
        landing.append((
            jnp.where(arriving > 0, slots_ref[2, m, anchor], -1),
            [jnp.where(arriving > 0, blocks_ref[m, 1, j, anchor], -1) for j in range(per_request)],
        ))

    @pl.loop(0, s_all.shape[0])
    def _(s):
        value = s_all[s]
        for m in range(moves):
            value = lax.select(leaving[m][0] == s, jnp.zeros_like(value), value)
        for m in range(moves):
            moved = jnp.concatenate([pay[bits, m, i] for i in range(pieces)], axis=1)
            value = lax.select(landing[m][0] == s, moved, value)
        new_states[s] = value

    @pl.loop(0, c_all.shape[0])
    def _(s):
        value = c_all[s]
        for m in range(moves):
            for j in range(per_request):
                value = lax.select(leaving[m][1][j] == s, jnp.zeros_like(value), value)
        for m in range(moves):
            for j in range(per_request):
                value = lax.select(landing[m][1][j] == s, pay[bits, m, pl.ds(pieces + 2 * j, 2)], value)
        new_cache[s] = value

    for n in range(early, len(groups)):
        mix(n)

    for step in range(bits):
        pltpu.make_async_copy(pay.at[step], pay.at[step], mig_send).wait()
    most = packed_ref.at[:, pl.ds(0, ranks - 1)]
    pltpu.make_async_copy(most, most, first_send).wait()
    most = x_in.at[:, 0]
    pltpu.make_async_copy(most, most, cross_send).wait()
    most = x_in.at[:, pl.ds(0, 2)]
    pltpu.make_async_copy(most, most, pair_send).wait()
    for _, pair, home in stores:
        pltpu.make_async_copy(pair.at[0], pair.at[0], half_send).wait()
        most = home.at[0, :, pl.ds(0, owners - 1)]
        pltpu.make_async_copy(most, most, back_send).wait()


def fused(
    tokens, router, expert_ids, w_gate, w_up, w_down, states, kv_blocks,
    plan_slots, plan_len, plan_blocks,
):
    ranks, quads = lax.axis_size("dp"), lax.axis_size("ep")
    experts = router.shape[1]
    tok_count, width = tokens.shape
    moves = plan_slots.shape[1]
    per_request = plan_blocks.shape[3]
    bf16 = jnp.bfloat16
    dma = pltpu.SemaphoreType.DMA
    like = jax.ShapeDtypeStruct
    ids = expert_ids.T
    slots = jnp.transpose(plan_slots, (2, 1, 0))
    lengths = plan_len.T
    blocks = jnp.transpose(plan_blocks, (1, 2, 3, 0))
    routes = router.T
    depth = w_gate.shape[2]
    down_tiles = width // (2 * TILE)
    owners = 2 * ranks
    bits = ranks.bit_length() - 1
    slim = 2 + down_tiles % 2
    wide = (down_tiles - slim) // 2
    lanes = kv_blocks.shape[3]
    request = (states.shape[2] // lanes + per_request * kv_blocks.shape[1], *kv_blocks.shape[2:])
    outputs = pl.pallas_call(
        functools.partial(expert_kernel, ranks, quads),
        out_shape=(
            pltpu.VMEM(states.shape, bf16),
            pltpu.VMEM(kv_blocks.shape, bf16),
            pltpu.VMEM(tokens.shape, bf16),
        ),
        in_specs=[ANY] * 11,
        out_specs=(VMEM, VMEM, VMEM),
        scratch_shapes=[
            pltpu.SMEM(ids.shape, jnp.int32),
            pltpu.SMEM(slots.shape, jnp.int32),
            pltpu.SMEM(lengths.shape, jnp.int32),
            pltpu.SMEM(blocks.shape, jnp.int32),
            pltpu.VMEM(tokens.shape, bf16),
            pltpu.VMEM(routes.shape, jnp.float32),
            pltpu.VMEM((PARTS, experts, CAP, width // PARTS), bf16),
            pltpu.VMEM(states.shape, bf16),
            pltpu.VMEM(kv_blocks.shape, bf16),
            pltpu.VMEM((bits + 1, moves, *request), bf16),
            pltpu.VMEM((bits, moves, *request), bf16),
            pltpu.VMEM((RING, 2, width, TILE), bf16),
            pltpu.VMEM((PARTS, quads, ranks, CAP, width // PARTS), bf16),
            pltpu.VMEM((quads * ranks * CAP, width), bf16),
            pltpu.VMEM((SPLIT * WIDE, 2, quads * ranks * CAP, TILE), jnp.float32),
            pltpu.VMEM((quads * ranks * CAP, depth), bf16),
            *[
                spec
                for count, columns in ((wide, 4 * TILE), (slim, 2 * TILE))
                for spec in (
                    pltpu.VMEM((count, owners * CAP, columns), jnp.float32),
                    pltpu.VMEM((2, count, owners * CAP, columns), jnp.float32),
                    pltpu.VMEM((2, count, owners, CAP, columns), bf16),
                )
            ],
            dma((6,)), dma((2,)), dma((RING,)), dma, dma((PARTS, ranks)), dma, dma((PARTS, ranks)),
            dma, dma((PARTS,)),
            dma, dma((wide + slim,)), dma, dma((wide + slim,)), dma, dma((bits,)),
        ],
        compiler_params=pltpu.CompilerParams(
            collective_id=0, has_side_effects=True, vmem_limit_bytes=VMEM_LIMIT
        ),
        name="expert",
    )(
        ids, slots, lengths, blocks, tokens, routes, w_gate, w_up, w_down, states, kv_blocks
    )
    outputs = [pltpu.with_memory_space_constraint(o, pltpu.VMEM) for o in outputs]
    new_states, new_cache, mixed = pl.pallas_call(
        land_kernel,
        out_shape=(like(states.shape, bf16), like(kv_blocks.shape, bf16), like(tokens.shape, bf16)),
        in_specs=[VMEM] * 3,
        out_specs=(ANY, ANY, ANY),
        scratch_shapes=[dma((3,))],
        compiler_params=pltpu.CompilerParams(vmem_limit_bytes=LAND_LIMIT),
        name="land",
    )(*outputs)
    return mixed, new_states, new_cache


def local(
    tokens,
    router,
    expert_ids,
    w_gate,
    w_up,
    w_down,
    states,
    kv_blocks,
    plan_slots,
    plan_len,
    plan_blocks,
):
    ranks = lax.axis_size("dp")
    here = lax.axis_index("dp")
    moves = plan_slots.shape[1]
    slot_count = states.shape[0]
    block_count = kv_blocks.shape[0]
    per_request = plan_blocks.shape[3]
    block_len = kv_blocks.shape[2]
    mine = lax.dynamic_index_in_dim(plan_slots, here, 0, keepdims=False)
    my_blocks = lax.dynamic_index_in_dim(plan_blocks, here, 0, keepdims=False)
    my_length = lax.dynamic_index_in_dim(plan_len, here, 0, keepdims=False)
    leaving_slot = mine[:, 0]
    leaving_block = my_blocks[:, 0, :]
    state_out = states[jnp.maximum(leaving_slot, 0)]
    state_out = jnp.where((leaving_slot >= 0)[:, None, None], state_out, jnp.zeros_like(state_out))
    cache_out = kv_blocks[jnp.maximum(leaving_block, 0)]
    position = jnp.arange(per_request)[:, None] * block_len + jnp.arange(block_len)[None, :]
    written = (leaving_block >= 0)[:, :, None] & (position[None] < my_length[:, None, None])
    cache_out = jnp.where(written[:, :, None, :, None], cache_out, jnp.zeros_like(cache_out))
    arrivals = plan_slots[:, :, 1] == here
    sender = jnp.sum(jnp.where(arrivals, jnp.arange(ranks)[:, None], 0), axis=0)
    arriving = jnp.any(arrivals, axis=0)
    peers = jnp.arange(ranks)
    match = mine[:, 1][None, :] == peers[:, None]
    which = jnp.sum(jnp.where(match, jnp.arange(moves)[None, :], 0), axis=1)
    filled = jnp.any(match, axis=1)
    send_state = jnp.where(
        filled[:, None, None], state_out[which], jnp.zeros_like(state_out[which])
    )
    send_cache = jnp.where(
        filled[:, None, None, None, None], cache_out[which], jnp.zeros_like(cache_out[which])
    )
    got_state, got_cache = (
        lax.all_to_all(send_state, "dp", split_axis=0, concat_axis=0, tiled=True),
        lax.all_to_all(send_cache, "dp", split_axis=0, concat_axis=0, tiled=True),
    )
    state_in = got_state[sender]
    cache_in = got_cache[sender]
    slot_line = jnp.arange(slot_count)
    gone = jnp.any(slot_line[:, None] == leaving_slot[None, :], axis=1)
    new_states = jnp.where(gone[:, None, None], jnp.zeros_like(states), states)
    block_line = jnp.arange(block_count)
    gone_blocks = jnp.any(block_line[:, None, None] == leaving_block[None], axis=(1, 2))
    new_cache = jnp.where(gone_blocks[:, None, None, None], jnp.zeros_like(kv_blocks), kv_blocks)
    for move_index in range(moves):
        anchor = sender[move_index]
        place = plan_slots[anchor, move_index, 2]
        landing = (slot_line == place) & arriving[move_index]
        new_states = jnp.where(landing[:, None, None], state_in[move_index][None], new_states)
        for block_index in range(per_request):
            spot = plan_blocks[anchor, move_index, 1, block_index]
            block_hit = (block_line == spot) & arriving[move_index]
            new_cache = jnp.where(
                block_hit[:, None, None, None], cache_in[move_index, block_index][None], new_cache
            )
    experts = router.shape[1]
    tok_count = tokens.shape[0]
    width = tokens.shape[1]
    group = ranks // experts
    flat_ids = expert_ids.reshape(-1)
    onehot = (flat_ids[:, None] == jnp.arange(experts)[None, :]).astype(jnp.int32)
    earlier = jnp.cumsum(onehot, axis=0) - onehot
    slot_of = jnp.sum(earlier * onehot, axis=1)
    target_row = flat_ids * CAP + slot_of
    placer = (jnp.arange(experts * CAP)[:, None] == target_row[None, :]).astype(jnp.bfloat16)
    doubled = jnp.repeat(tokens, 2, axis=0)
    packed = jnp.dot(placer, doubled, preferred_element_type=jnp.float32).astype(jnp.bfloat16)
    outgoing = jnp.repeat(packed.reshape(experts, CAP, width), group, axis=0)
    incoming = lax.all_to_all(outgoing, "dp", split_axis=0, concat_axis=0, tiled=True)
    rows_in = incoming.reshape(ranks * CAP, width)
    piece = lax.all_gather(rows_in, "ep", axis=0, tiled=True)
    gate = jnp.dot(piece, w_gate[0], preferred_element_type=jnp.float32)
    upper = jnp.dot(piece, w_up[0], preferred_element_type=jnp.float32)
    hidden = (jax.nn.silu(gate) * upper).astype(jnp.bfloat16)
    summed = lax.psum_scatter(
        jnp.dot(hidden, w_down[0], preferred_element_type=jnp.float32),
        "ep",
        scatter_dimension=0,
        tiled=True,
    )
    returned = lax.all_to_all(
        summed.reshape(ranks, CAP, width), "dp", split_axis=0, concat_axis=0, tiled=True
    )
    expert_out = jnp.sum(returned.reshape(experts, group, CAP, width), axis=1).reshape(
        experts * CAP, width
    )
    chosen = expert_out[target_row].reshape(tok_count, 2, width)
    logits = jnp.dot(tokens.astype(jnp.float32), router, precision=lax.Precision.HIGHEST)
    scores = jax.nn.sigmoid(jnp.take_along_axis(logits, expert_ids, axis=1))
    weights = scores / jnp.sum(scores, axis=1, keepdims=True)
    mixed = jnp.sum(weights[:, :, None] * chosen, axis=1).astype(jnp.bfloat16)
    return (mixed, new_states, new_cache)


def solution(mesh):
    placed = (
        P(("dp", "ep"), None),
        P(),
        P(("dp", "ep"), None),
        P("dp", None, "ep"),
        P("dp", None, "ep"),
        P("dp", "ep", None),
        P("dp", None, "ep"),
        P("dp", None, None, "ep"),
        P(),
        P(),
        P(),
    )
    def step(*args):
        ranks, quads = lax.axis_size("dp"), lax.axis_size("ep")
        one_slab = args[1].shape[1] == ranks and ranks & (ranks - 1) == 0
        two_by_two = quads == 2 * 2
        return (fused if one_slab and two_by_two else local)(*args)

    return jax.shard_map(
        step,
        mesh=mesh,
        in_specs=placed,
        out_specs=(P(("dp", "ep"), None), P("dp", None, "ep"), P("dp", None, None, "ep")),
        check_vma=False,
    )
```

```python
import functools

import jax
import jax.numpy as jnp
from jax import lax
from jax.experimental import pallas as pl
from jax.experimental.pallas import tpu as pltpu
from jax.sharding import PartitionSpec as P

CAP = 2
MESH = pl.DeviceIdType.MESH
ANY = pl.BlockSpec(memory_space=pl.ANY)
VMEM = pl.BlockSpec(memory_space=pltpu.VMEM)
SMEM = pl.BlockSpec(memory_space=pltpu.SMEM)
VMEM_LIMIT = 65_000_000
TILE = 256
RING = 13
EARLY = 2
WIDE = 3
PARTS = 2
SPLIT = 6
LAND_LIMIT = 1 << 20


def target_rows(ids_ref, tok_count):
    picks = [ids_ref[k, t] for t in range(tok_count) for k in range(2)]
    rows = []
    for p, expert in enumerate(picks):
        slot = jnp.int32(0)
        for q in range(p):
            slot = slot + jnp.where(picks[q] == expert, 1, 0)
        rows.append(expert * CAP + slot)
    return picks, rows


def land_kernel(states_ref, cache_ref, mixed_ref, new_states, new_cache, new_mixed, sem):
    pairs = ((states_ref, new_states), (cache_ref, new_cache), (mixed_ref, new_mixed))
    copies = [pltpu.make_async_copy(a, b, sem.at[i]) for i, (a, b) in enumerate(pairs)]
    for copy in copies:
        copy.start()
    for copy in copies:
        copy.wait()


def expert_kernel(
    ranks, quads,
    ids_hbm, slots_hbm, len_hbm, blocks_hbm, tok_hbm, router_hbm, gate_ref, up_ref, down_ref,
    states_ref, kv_ref,
    new_states, new_cache, mixed_ref,
    ids_ref, slots_ref, len_ref, blocks_ref, tok_ref, router_ref,
    packed_ref, s_all, c_all, pay, got,
    w_buf, x_in, x_all, part_sum, hidden, wide_keep, wide_pair, wide_home, slim_keep, slim_pair, slim_home,
    small_sem, big_sem, w_sem, first_send, first_recv, cross_send, cross_recv, pair_send, pair_recv,
    half_send, half_recv, back_send, back_recv, mig_send, mig_recv,
):
    d = lax.axis_index("dp")
    e = lax.axis_index("ep")
    side, core = e // 2, lax.rem(e, 2)
    across, twin = (1 - side) * 2 + core, side * 2 + 1 - core
    diagonal = (1 - side) * 2 + 1 - core
    experts = ranks
    up_tiles = gate_ref.shape[2] // TILE
    down_tiles = down_ref.shape[2] // (2 * TILE)
    depth = down_ref.shape[1]
    ring = w_buf.shape[0]
    rows_half = 2 * ranks * CAP
    owners = 2 * ranks
    span = packed_ref.shape[3]
    me = side * ranks + d

    barrier = pltpu.get_barrier_semaphore()

    z_count = ranks // 2

    def planes(i, reverse):
        forward = (d // 2 < z_count // 2) == (not reverse)
        return jnp.where(forward, i, z_count - 1 - i)

    for i in range(z_count):
        for flip in range(2):
            other = planes(i, True) * 2 + lax.rem(d + 1 + flip, 2)

            @pl.when(other != d)
            def _():
                pl.semaphore_signal(barrier, inc=1, device_id=(other, e), device_id_type=MESH)

    for quad in (across, diagonal, twin):
        pl.semaphore_signal(barrier, inc=1, device_id=(d, quad), device_id_type=MESH)

    smalls = [
        pltpu.make_async_copy(a, b, small_sem.at[i])
        for i, (a, b) in enumerate((
            (tok_hbm, tok_ref), (ids_hbm, ids_ref), (router_hbm, router_ref),
            (slots_hbm, slots_ref), (len_hbm, len_ref), (blocks_hbm, blocks_ref),
        ))
    ]
    for copy in smalls:
        copy.start()

    def up_copies(j):
        columns = pl.ds(pl.multiple_of(j * TILE, TILE), TILE)
        return (
            pltpu.make_async_copy(gate_ref.at[0, :, columns], w_buf.at[j, 0], w_sem.at[j]),
            pltpu.make_async_copy(up_ref.at[0, :, columns], w_buf.at[j, 1], w_sem.at[j]),
        )

    def up_wait(j):
        pltpu.make_async_copy(w_buf.at[j], w_buf.at[j], w_sem.at[j]).wait()

    def down_copies(c):
        slot = lax.rem(up_tiles + c, ring)
        found = []
        for h in range(2):
            columns = pl.ds(pl.multiple_of((2 * c + h) * TILE, TILE), TILE)
            found.append(pltpu.make_async_copy(
                down_ref.at[0, :, columns], w_buf.at[slot, h, pl.ds(0, depth)], w_sem.at[slot]
            ))
        return found

    def down_wait(c):
        slot = lax.rem(up_tiles + c, ring)
        both = w_buf.at[slot, :, pl.ds(0, depth)]
        pltpu.make_async_copy(both, both, w_sem.at[slot]).wait()

    load_states = pltpu.make_async_copy(states_ref, s_all, big_sem.at[0])
    load_cache = pltpu.make_async_copy(kv_ref, c_all, big_sem.at[1])

    @pl.loop(0, EARLY)
    def _(j):
        for copy in up_copies(j):
            copy.start()

    load_states.start()
    load_cache.start()

    @pl.loop(EARLY, up_tiles)
    def _(j):
        for copy in up_copies(j):
            copy.start()

    @pl.loop(0, ring - up_tiles)
    def _(c):
        for copy in down_copies(c):
            copy.start()

    smalls[0].wait()
    smalls[1].wait()
    tok_count = tok_ref.shape[0]
    picks, rows = target_rows(ids_ref, tok_count)
    row_at = lax.broadcasted_iota(jnp.int32, (experts * CAP, tok_count), 0)
    tok_at = lax.broadcasted_iota(jnp.int32, (experts * CAP, tok_count), 1)
    placer = jnp.zeros((experts * CAP, tok_count), jnp.float32)
    for p, row in enumerate(rows):
        placer = jnp.where((row_at == row) & (tok_at == p // 2), 1.0, placer)
    packed = jnp.dot(
        placer.astype(jnp.bfloat16), tok_ref[...], preferred_element_type=jnp.float32
    ).astype(jnp.bfloat16)
    for h in range(PARTS):
        for r in range(experts):
            packed_ref[h, r] = packed[r * CAP : (r + 1) * CAP, h * span : (h + 1) * span]
        x_in[h, e, d] = packed_ref[h, d]

    pl.semaphore_wait(barrier, ranks + 2)

    def cross(src, h, source):
        return pltpu.make_async_remote_copy(
            src, x_in.at[h, e, source], cross_send, cross_recv.at[h, source],
            device_id=(d, across), device_id_type=MESH,
        )

    def to_other(src, h, quad, source, where):
        return pltpu.make_async_remote_copy(
            src, x_in.at[h, quad, source], pair_send, pair_recv.at[h],
            device_id=(d, where), device_id_type=MESH,
        )

    def spread(src, h, source):
        cross(src, h, source).start()
        to_other(src, h, e, source, twin).start()

        @pl.when(core == 0)
        def _():
            to_other(src, h, e, source, diagonal).start()

    for h in range(PARTS):
        for i in range(z_count):
            plane = planes(i, True)
            for y in range(2):
                peer = plane * 2 + y

                @pl.when(peer != d)
                def _():
                    pltpu.make_async_remote_copy(
                        packed_ref.at[h, peer], x_in.at[h, e, d], first_send, first_recv.at[h, d],
                        device_id=(peer, e), device_id_type=MESH,
                    ).start()

        spread(packed_ref.at[h, d], h, d)

    smalls[2].wait()
    wide = tok_ref[...].astype(jnp.float32)
    lane = lax.broadcasted_iota(jnp.int32, (tok_count, experts), 1)
    seat = lax.broadcasted_iota(jnp.int32, (tok_count, experts), 0)
    logits = jnp.zeros((tok_count, experts), jnp.float32)
    for r in range(experts):
        product = jnp.sum(wide * router_ref[r : r + 1, :], axis=1, keepdims=True)
        logits = jnp.where(lane == r, product, logits)
    column = lax.broadcasted_iota(jnp.int32, (tok_count, owners * CAP), 1)
    token = lax.broadcasted_iota(jnp.int32, (tok_count, owners * CAP), 0)
    row_of = lax.rem(column, ranks * CAP)
    scores, hits = [], []
    for k in range(2):
        chosen = jnp.zeros(logits.shape, jnp.int32)
        target = jnp.zeros(column.shape, jnp.int32)
        for t in range(tok_count):
            chosen = jnp.where(seat == t, picks[2 * t + k], chosen)
            target = jnp.where(token == t, rows[2 * t + k], target)
        value = jnp.sum(jnp.where(lane == chosen, logits, 0.0), axis=1, keepdims=True)
        scores.append(jax.nn.sigmoid(value))
        hits.append(row_of == target)
    total = scores[0] + scores[1]
    comb = jnp.where(hits[0], scores[0] / total, 0.0) + jnp.where(hits[1], scores[1] / total, 0.0)
    comb_high = comb.astype(jnp.bfloat16)
    comb_low = (comb - comb_high.astype(jnp.float32)).astype(jnp.bfloat16)

    near = [planes(i, False) * 2 + y for i in range(z_count) for y in range(2)]

    def relay(h):
        for source in near:
            cross(x_in.at[h, across, source], h, source).wait_recv()

            @pl.when(core == 1)
            def _():
                to_other(x_in.at[h, across, source], h, across, source, twin).start()

    for h in range(PARTS):
        for source in near:

            @pl.when(source != d)
            def _():
                pltpu.make_async_remote_copy(
                    packed_ref.at[h, d], x_in.at[h, e, source], first_send, first_recv.at[h, source],
                    device_id=(source, e), device_id_type=MESH,
                ).wait_recv()
                spread(x_in.at[h, e, source], h, source)

    for copy in smalls[3:]:
        copy.wait()
    load_states.wait()
    load_cache.wait()
    moves = slots_ref.shape[1]
    per_request = blocks_ref.shape[2]
    block_len, lanes = kv_ref.shape[2:]
    pieces = states_ref.shape[2] // lanes
    position = lax.broadcasted_iota(jnp.int32, kv_ref.shape[1:], 1)
    for m in range(moves):
        state = s_all[jnp.maximum(slots_ref[0, m, d], 0)]
        for i in range(pieces):
            pay[0, m, i] = state[:, i * lanes : (i + 1) * lanes]
        for j in range(per_request):
            kept = c_all[jnp.maximum(blocks_ref[m, 0, j, d], 0)].astype(jnp.float32)
            kept = jnp.where(j * block_len + position < len_ref[m, d], kept, 0.0)
            pay[0, m, pl.ds(pieces + 2 * j, 2)] = kept.astype(jnp.bfloat16)
    shifts = []
    for m in range(moves):
        shift = jnp.int32(0)
        for r in range(ranks):
            gap = slots_ref[1, m, r] - r
            gap = gap + jnp.where(gap < 0, ranks, 0)
            shift = jnp.where(slots_ref[1, m, r] >= 0, gap, shift)
        shifts.append(shift)
    bits = ranks.bit_length() - 1

    def bit_of(m, step):
        return 0 if step == bits - 1 else bits - 1 - (step + m) % (bits - 1)

    def hop_copy(m, step):
        bit = 1 << bit_of(m, step)
        peer = d + bit - 2 * bit * lax.rem(d // bit, 2)
        return pltpu.make_async_remote_copy(
            pay.at[step, m], got.at[step, m], mig_send, mig_recv.at[step],
            device_id=(peer, e), device_id_type=MESH,
        )

    def hop_start(step):
        for m in range(moves):
            hop_copy(m, step).start()

    def hop_finish(step):
        pltpu.make_async_copy(got.at[step], got.at[step], mig_recv.at[step]).wait()
        for m in range(moves):
            bit = 1 << bit_of(m, step)
            fixed = sum(1 << bit_of(m, s) for s in range(step + 1))
            loose = ranks - 1 - fixed
            swap = jnp.int32(0)
            for r in range(ranks):
                reach = (r + shifts[m]) & (ranks - 1)
                held = (((d ^ r) & loose) | ((d ^ reach) & fixed)) == 0
                swap = jnp.where(held & (((d ^ r) & bit) != 0), 1, swap)
            pay[step + 1, m] = lax.select(swap > 0, got[step, m], pay[step, m])

    hop_start(0)
    relay(0)

    def gather(h, which):
        for half in range(2):
            at = pl.multiple_of((which * 2 + half) * ranks * CAP, ranks * CAP)
            x_all[pl.ds(at, ranks * CAP), h * span : (h + 1) * span] = jnp.concatenate(
                [x_in[h, half * 2 + which, r] for r in range(ranks)], axis=0
            )

    def pair_wait(h):
        most = x_in.at[h, pl.ds(0, 2)]
        pltpu.make_async_copy(most, most, pair_recv.at[h]).wait()

    gather(0, core)
    pair_wait(0)
    gather(0, 1 - core)

    def product(j, which, h):
        rows_of = pl.ds(h * span, span)
        return jnp.dot(x_all[:, rows_of], w_buf[j, which, rows_of], preferred_element_type=jnp.float32)

    def finish_up(j, gate, upper):
        value = gate / (1.0 + jnp.exp(-gate)) * upper
        hidden[:, j * TILE : (j + 1) * TILE] = value.astype(jnp.bfloat16)

    def refill(j):
        later = j + ring - up_tiles

        if later < down_tiles:
            for copy in down_copies(later):
                copy.start()

    def first_step(tiles):
        for j in tiles:
            up_wait(j)
        for j in tiles:
            for which in range(2):
                part_sum[j, which] = product(j, which, 0)

    def second_step(tiles):
        for j in tiles:
            sums = [part_sum[j, which] for which in range(2)]
            for h in range(1, PARTS):
                sums = [sums[which] + product(j, which, h) for which in range(2)]
            finish_up(j, *sums)
        for j in tiles:
            refill(j)

    def whole_step(tiles):
        for j in tiles:
            up_wait(j)
        for j in tiles:
            gate, upper = [
                jnp.dot(x_all[...], w_buf[j, which], preferred_element_type=jnp.float32)
                for which in range(2)
            ]
            finish_up(j, gate, upper)
        for j in tiles:
            refill(j)

    split = part_sum.shape[0]
    early = split - 2
    first_step(range(early))
    for h in range(1, PARTS):
        relay(h)
        gather(h, core)
    first_step(range(early, split))
    for h in range(1, PARTS):
        pair_wait(h)
        gather(h, 1 - core)
    for start in range(0, split, WIDE):
        second_step(range(start, min(start + WIDE, split)))
        if start == 0:
            hop_finish(0)
            hop_start(1)
    for start in range(split, up_tiles, WIDE):
        whole_step(range(start, min(start + WIDE, up_tiles)))
    wide_count = wide_keep.shape[0]
    groups = [(0, g, 2 * g, 2) for g in range(wide_count)]
    groups += [(1, g, 2 * wide_count + g, 1) for g in range(slim_keep.shape[0])]
    stores = ((wide_keep, wide_pair, wide_home), (slim_keep, slim_pair, slim_home))

    def swap_copy(n):
        kind, g, _, _ = groups[n]
        pair = stores[kind][1]
        return pltpu.make_async_remote_copy(
            pair.at[0, g], pair.at[1, g], half_send, half_recv.at[n],
            device_id=(d, twin), device_id_type=MESH,
        )

    def send_home(n):
        kind, g, _, _ = groups[n]
        keep, pair, home = stores[kind]
        swap_copy(n).wait_recv()
        whole = (keep[g] + pair[1, g]).astype(jnp.bfloat16)
        for o in range(owners):
            home[0, g, o] = whole[o * CAP : (o + 1) * CAP]
        home[1, g, me] = home[0, g, me]

        @pl.loop(1, owners, unroll=True)
        def _(k):
            other = lax.rem(me + k, owners)
            pltpu.make_async_remote_copy(
                home.at[0, g, other], home.at[1, g, me], back_send, back_recv.at[n],
                device_id=(lax.rem(other, ranks), (other // ranks) * 2 + core), device_id_type=MESH,
            ).start()

    def multiply(n):
        kind, g, start, count = groups[n]
        keep, pair, _ = stores[kind]
        for c in range(start, start + count):
            down_wait(c)
        for c in range(start, start + count):
            slot = lax.rem(up_tiles + c, ring)
            for h in range(2):
                part = jnp.dot(
                    hidden[...], w_buf[slot, h, pl.ds(0, depth)], preferred_element_type=jnp.float32
                )
                low, high = part[:rows_half], part[rows_half:]
                first = core == 0
                columns = pl.ds((2 * (c - start) + h) * TILE, TILE)
                keep[g, :, columns] = lax.select(first, low, high)
                pair[0, g, :, columns] = lax.select(first, high, low)
        swap_copy(n).start()

    def mix(n):
        kind, g, start, count = groups[n]
        home = stores[kind][2]
        most = home.at[1, g, pl.ds(0, owners - 1)]
        pltpu.make_async_copy(most, most, back_recv.at[n]).wait()
        rows_in = jnp.concatenate([home[1, g, o] for o in range(owners)], axis=0)
        high = jnp.dot(comb_high, rows_in, preferred_element_type=jnp.float32)
        low = jnp.dot(comb_low, rows_in, preferred_element_type=jnp.float32)
        mixed_ref[:, start * 2 * TILE : (start + count) * 2 * TILE] = (high + low).astype(jnp.bfloat16)

    for n in range(len(groups)):
        multiply(n)
        if n > 0:
            send_home(n - 1)
        else:
            for step in range(1, bits - 1):
                hop_finish(step)
                hop_start(step + 1)
    send_home(len(groups) - 1)
    mixed_early = max(len(groups) - 2, 0)
    for n in range(mixed_early):
        mix(n)
    hop_finish(bits - 1)

    leaving, landing = [], []
    for m in range(moves):
        anchor, arriving = jnp.int32(0), jnp.int32(0)
        for r in range(ranks):
            hit = slots_ref[1, m, r] == d
            anchor = jnp.where(hit, r, anchor)
            arriving = jnp.where(hit, 1, arriving)
        leaving.append((slots_ref[0, m, d], [blocks_ref[m, 0, j, d] for j in range(per_request)]))
        landing.append((
            jnp.where(arriving > 0, slots_ref[2, m, anchor], -1),
            [jnp.where(arriving > 0, blocks_ref[m, 1, j, anchor], -1) for j in range(per_request)],
        ))

    @pl.loop(0, s_all.shape[0])
    def _(s):
        value = s_all[s]
        for m in range(moves):
            value = lax.select(leaving[m][0] == s, jnp.zeros_like(value), value)
        for m in range(moves):
            moved = jnp.concatenate([pay[bits, m, i] for i in range(pieces)], axis=1)
            value = lax.select(landing[m][0] == s, moved, value)
        new_states[s] = value

    @pl.loop(0, c_all.shape[0])
    def _(s):
        value = c_all[s]
        for m in range(moves):
            for j in range(per_request):
                value = lax.select(leaving[m][1][j] == s, jnp.zeros_like(value), value)
        for m in range(moves):
            for j in range(per_request):
                value = lax.select(landing[m][1][j] == s, pay[bits, m, pl.ds(pieces + 2 * j, 2)], value)
        new_cache[s] = value

    for n in range(mixed_early, len(groups)):
        mix(n)

    for step in range(bits):
        pltpu.make_async_copy(pay.at[step], pay.at[step], mig_send).wait()
    most = packed_ref.at[:, pl.ds(0, ranks - 1)]
    pltpu.make_async_copy(most, most, first_send).wait()
    most = x_in.at[:, 0]
    pltpu.make_async_copy(most, most, cross_send).wait()
    most = x_in.at[:, pl.ds(0, 2)]
    pltpu.make_async_copy(most, most, pair_send).wait()
    for _, pair, home in stores:
        pltpu.make_async_copy(pair.at[0], pair.at[0], half_send).wait()
        most = home.at[0, :, pl.ds(0, owners - 1)]
        pltpu.make_async_copy(most, most, back_send).wait()


def fused(
    tokens, router, expert_ids, w_gate, w_up, w_down, states, kv_blocks,
    plan_slots, plan_len, plan_blocks,
):
    ranks, quads = lax.axis_size("dp"), lax.axis_size("ep")
    experts = router.shape[1]
    tok_count, width = tokens.shape
    moves = plan_slots.shape[1]
    per_request = plan_blocks.shape[3]
    bf16 = jnp.bfloat16
    dma = pltpu.SemaphoreType.DMA
    like = jax.ShapeDtypeStruct
    ids = expert_ids.T
    slots = jnp.transpose(plan_slots, (2, 1, 0))
    lengths = plan_len.T
    blocks = jnp.transpose(plan_blocks, (1, 2, 3, 0))
    routes = router.T
    depth = w_gate.shape[2]
    down_tiles = width // (2 * TILE)
    owners = 2 * ranks
    bits = ranks.bit_length() - 1
    slim = 2 + down_tiles % 2
    wide = (down_tiles - slim) // 2
    lanes = kv_blocks.shape[3]
    request = (states.shape[2] // lanes + per_request * kv_blocks.shape[1], *kv_blocks.shape[2:])
    outputs = pl.pallas_call(
        functools.partial(expert_kernel, ranks, quads),
        out_shape=(
            pltpu.VMEM(states.shape, bf16),
            pltpu.VMEM(kv_blocks.shape, bf16),
            pltpu.VMEM(tokens.shape, bf16),
        ),
        in_specs=[ANY] * 11,
        out_specs=(VMEM, VMEM, VMEM),
        scratch_shapes=[
            pltpu.SMEM(ids.shape, jnp.int32),
            pltpu.SMEM(slots.shape, jnp.int32),
            pltpu.SMEM(lengths.shape, jnp.int32),
            pltpu.SMEM(blocks.shape, jnp.int32),
            pltpu.VMEM(tokens.shape, bf16),
            pltpu.VMEM(routes.shape, jnp.float32),
            pltpu.VMEM((PARTS, experts, CAP, width // PARTS), bf16),
            pltpu.VMEM(states.shape, bf16),
            pltpu.VMEM(kv_blocks.shape, bf16),
            pltpu.VMEM((bits + 1, moves, *request), bf16),
            pltpu.VMEM((bits, moves, *request), bf16),
            pltpu.VMEM((RING, 2, width, TILE), bf16),
            pltpu.VMEM((PARTS, quads, ranks, CAP, width // PARTS), bf16),
            pltpu.VMEM((quads * ranks * CAP, width), bf16),
            pltpu.VMEM((SPLIT, 2, quads * ranks * CAP, TILE), jnp.float32),
            pltpu.VMEM((quads * ranks * CAP, depth), bf16),
            *[
                spec
                for count, columns in ((wide, 4 * TILE), (slim, 2 * TILE))
                for spec in (
                    pltpu.VMEM((count, owners * CAP, columns), jnp.float32),
                    pltpu.VMEM((2, count, owners * CAP, columns), jnp.float32),
                    pltpu.VMEM((2, count, owners, CAP, columns), bf16),
                )
            ],
            dma((6,)), dma((2,)), dma((RING,)), dma, dma((PARTS, ranks)), dma, dma((PARTS, ranks)),
            dma, dma((PARTS,)),
            dma, dma((wide + slim,)), dma, dma((wide + slim,)), dma, dma((bits,)),
        ],
        compiler_params=pltpu.CompilerParams(
            collective_id=0, has_side_effects=True, vmem_limit_bytes=VMEM_LIMIT
        ),
        name="expert",
    )(
        ids, slots, lengths, blocks, tokens, routes, w_gate, w_up, w_down, states, kv_blocks
    )
    outputs = [pltpu.with_memory_space_constraint(o, pltpu.VMEM) for o in outputs]
    new_states, new_cache, mixed = pl.pallas_call(
        land_kernel,
        out_shape=(like(states.shape, bf16), like(kv_blocks.shape, bf16), like(tokens.shape, bf16)),
        in_specs=[VMEM] * 3,
        out_specs=(ANY, ANY, ANY),
        scratch_shapes=[dma((3,))],
        compiler_params=pltpu.CompilerParams(vmem_limit_bytes=LAND_LIMIT),
        name="land",
    )(*outputs)
    return mixed, new_states, new_cache


def local(
    tokens,
    router,
    expert_ids,
    w_gate,
    w_up,
    w_down,
    states,
    kv_blocks,
    plan_slots,
    plan_len,
    plan_blocks,
):
    ranks = lax.axis_size("dp")
    here = lax.axis_index("dp")
    moves = plan_slots.shape[1]
    slot_count = states.shape[0]
    block_count = kv_blocks.shape[0]
    per_request = plan_blocks.shape[3]
    block_len = kv_blocks.shape[2]
    mine = lax.dynamic_index_in_dim(plan_slots, here, 0, keepdims=False)
    my_blocks = lax.dynamic_index_in_dim(plan_blocks, here, 0, keepdims=False)
    my_length = lax.dynamic_index_in_dim(plan_len, here, 0, keepdims=False)
    leaving_slot = mine[:, 0]
    leaving_block = my_blocks[:, 0, :]
    state_out = states[jnp.maximum(leaving_slot, 0)]
    state_out = jnp.where((leaving_slot >= 0)[:, None, None], state_out, jnp.zeros_like(state_out))
    cache_out = kv_blocks[jnp.maximum(leaving_block, 0)]
    position = jnp.arange(per_request)[:, None] * block_len + jnp.arange(block_len)[None, :]
    written = (leaving_block >= 0)[:, :, None] & (position[None] < my_length[:, None, None])
    cache_out = jnp.where(written[:, :, None, :, None], cache_out, jnp.zeros_like(cache_out))
    arrivals = plan_slots[:, :, 1] == here
    sender = jnp.sum(jnp.where(arrivals, jnp.arange(ranks)[:, None], 0), axis=0)
    arriving = jnp.any(arrivals, axis=0)
    peers = jnp.arange(ranks)
    match = mine[:, 1][None, :] == peers[:, None]
    which = jnp.sum(jnp.where(match, jnp.arange(moves)[None, :], 0), axis=1)
    filled = jnp.any(match, axis=1)
    send_state = jnp.where(
        filled[:, None, None], state_out[which], jnp.zeros_like(state_out[which])
    )
    send_cache = jnp.where(
        filled[:, None, None, None, None], cache_out[which], jnp.zeros_like(cache_out[which])
    )
    got_state, got_cache = (
        lax.all_to_all(send_state, "dp", split_axis=0, concat_axis=0, tiled=True),
        lax.all_to_all(send_cache, "dp", split_axis=0, concat_axis=0, tiled=True),
    )
    state_in = got_state[sender]
    cache_in = got_cache[sender]
    slot_line = jnp.arange(slot_count)
    gone = jnp.any(slot_line[:, None] == leaving_slot[None, :], axis=1)
    new_states = jnp.where(gone[:, None, None], jnp.zeros_like(states), states)
    block_line = jnp.arange(block_count)
    gone_blocks = jnp.any(block_line[:, None, None] == leaving_block[None], axis=(1, 2))
    new_cache = jnp.where(gone_blocks[:, None, None, None], jnp.zeros_like(kv_blocks), kv_blocks)
    for move_index in range(moves):
        anchor = sender[move_index]
        place = plan_slots[anchor, move_index, 2]
        landing = (slot_line == place) & arriving[move_index]
        new_states = jnp.where(landing[:, None, None], state_in[move_index][None], new_states)
        for block_index in range(per_request):
            spot = plan_blocks[anchor, move_index, 1, block_index]
            block_hit = (block_line == spot) & arriving[move_index]
            new_cache = jnp.where(
                block_hit[:, None, None, None], cache_in[move_index, block_index][None], new_cache
            )
    experts = router.shape[1]
    tok_count = tokens.shape[0]
    width = tokens.shape[1]
    group = ranks // experts
    flat_ids = expert_ids.reshape(-1)
    onehot = (flat_ids[:, None] == jnp.arange(experts)[None, :]).astype(jnp.int32)
    earlier = jnp.cumsum(onehot, axis=0) - onehot
    slot_of = jnp.sum(earlier * onehot, axis=1)
    target_row = flat_ids * CAP + slot_of
    placer = (jnp.arange(experts * CAP)[:, None] == target_row[None, :]).astype(jnp.bfloat16)
    doubled = jnp.repeat(tokens, 2, axis=0)
    packed = jnp.dot(placer, doubled, preferred_element_type=jnp.float32).astype(jnp.bfloat16)
    outgoing = jnp.repeat(packed.reshape(experts, CAP, width), group, axis=0)
    incoming = lax.all_to_all(outgoing, "dp", split_axis=0, concat_axis=0, tiled=True)
    rows_in = incoming.reshape(ranks * CAP, width)
    piece = lax.all_gather(rows_in, "ep", axis=0, tiled=True)
    gate = jnp.dot(piece, w_gate[0], preferred_element_type=jnp.float32)
    upper = jnp.dot(piece, w_up[0], preferred_element_type=jnp.float32)
    hidden = (jax.nn.silu(gate) * upper).astype(jnp.bfloat16)
    summed = lax.psum_scatter(
        jnp.dot(hidden, w_down[0], preferred_element_type=jnp.float32),
        "ep",
        scatter_dimension=0,
        tiled=True,
    )
    returned = lax.all_to_all(
        summed.reshape(ranks, CAP, width), "dp", split_axis=0, concat_axis=0, tiled=True
    )
    expert_out = jnp.sum(returned.reshape(experts, group, CAP, width), axis=1).reshape(
        experts * CAP, width
    )
    chosen = expert_out[target_row].reshape(tok_count, 2, width)
    logits = jnp.dot(tokens.astype(jnp.float32), router, precision=lax.Precision.HIGHEST)
    scores = jax.nn.sigmoid(jnp.take_along_axis(logits, expert_ids, axis=1))
    weights = scores / jnp.sum(scores, axis=1, keepdims=True)
    mixed = jnp.sum(weights[:, :, None] * chosen, axis=1).astype(jnp.bfloat16)
    return (mixed, new_states, new_cache)


def solution(mesh):
    placed = (
        P(("dp", "ep"), None),
        P(),
        P(("dp", "ep"), None),
        P("dp", None, "ep"),
        P("dp", None, "ep"),
        P("dp", "ep", None),
        P("dp", None, "ep"),
        P("dp", None, None, "ep"),
        P(),
        P(),
        P(),
    )
    def step(*args):
        ranks, quads = lax.axis_size("dp"), lax.axis_size("ep")
        one_slab = args[1].shape[1] == ranks and ranks & (ranks - 1) == 0
        two_by_two = quads == 2 * 2
        return (fused if one_slab and two_by_two else local)(*args)

    return jax.shard_map(
        step,
        mesh=mesh,
        in_specs=placed,
        out_specs=(P(("dp", "ep"), None), P("dp", None, "ep"), P("dp", None, None, "ep")),
        check_vma=False,
    )
```

```python
import functools

import jax
import jax.numpy as jnp
from jax import lax
from jax.experimental import pallas as pl
from jax.experimental.pallas import tpu as pltpu
from jax.sharding import PartitionSpec as P

CAP = 2
MESH = pl.DeviceIdType.MESH
ANY = pl.BlockSpec(memory_space=pl.ANY)
VMEM = pl.BlockSpec(memory_space=pltpu.VMEM)
SMEM = pl.BlockSpec(memory_space=pltpu.SMEM)
VMEM_LIMIT = 65_000_000
TILE = 256
RING = 13
EARLY = 2
WIDE = 3
PARTS = 2
SPLIT = 6
LAND_LIMIT = 1 << 20


def target_rows(ids_ref, tok_count):
    picks = [ids_ref[k, t] for t in range(tok_count) for k in range(2)]
    rows = []
    for p, expert in enumerate(picks):
        slot = jnp.int32(0)
        for q in range(p):
            slot = slot + jnp.where(picks[q] == expert, 1, 0)
        rows.append(expert * CAP + slot)
    return picks, rows


def land_kernel(states_ref, cache_ref, mixed_ref, new_states, new_cache, new_mixed, sem):
    pairs = ((states_ref, new_states), (cache_ref, new_cache), (mixed_ref, new_mixed))
    copies = [pltpu.make_async_copy(a, b, sem.at[i]) for i, (a, b) in enumerate(pairs)]
    for copy in copies:
        copy.start()
    for copy in copies:
        copy.wait()


def expert_kernel(
    ranks, quads,
    ids_hbm, slots_hbm, len_hbm, blocks_hbm, tok_hbm, router_hbm, gate_ref, up_ref, down_ref,
    states_ref, kv_ref,
    new_states, new_cache, mixed_ref,
    ids_ref, slots_ref, len_ref, blocks_ref, tok_ref, router_ref,
    packed_ref, s_all, c_all, pay, got,
    w_buf, x_in, x_all, part_sum, hidden, wide_keep, wide_pair, wide_home, slim_keep, slim_pair, slim_home,
    small_sem, big_sem, w_sem, first_send, first_recv, cross_send, cross_recv, pair_send, pair_recv,
    half_send, half_recv, back_send, back_recv, mig_send, mig_recv,
):
    d = lax.axis_index("dp")
    e = lax.axis_index("ep")
    side, core = e // 2, lax.rem(e, 2)
    across, twin = (1 - side) * 2 + core, side * 2 + 1 - core
    diagonal = (1 - side) * 2 + 1 - core
    experts = ranks
    up_tiles = gate_ref.shape[2] // TILE
    down_tiles = down_ref.shape[2] // (2 * TILE)
    depth = down_ref.shape[1]
    ring = w_buf.shape[0]
    rows_half = 2 * ranks * CAP
    owners = 2 * ranks
    span = packed_ref.shape[3]
    me = side * ranks + d

    barrier = pltpu.get_barrier_semaphore()

    z_count = ranks // 2

    def planes(i, reverse):
        forward = (d // 2 < z_count // 2) == (not reverse)
        return jnp.where(forward, i, z_count - 1 - i)

    for i in range(z_count):
        for flip in range(2):
            other = planes(i, True) * 2 + lax.rem(d + 1 + flip, 2)

            @pl.when(other != d)
            def _():
                pl.semaphore_signal(barrier, inc=1, device_id=(other, e), device_id_type=MESH)

    for quad in (across, diagonal, twin):
        pl.semaphore_signal(barrier, inc=1, device_id=(d, quad), device_id_type=MESH)

    smalls = [
        pltpu.make_async_copy(a, b, small_sem.at[i])
        for i, (a, b) in enumerate((
            (tok_hbm, tok_ref), (ids_hbm, ids_ref), (router_hbm, router_ref),
            (slots_hbm, slots_ref), (len_hbm, len_ref), (blocks_hbm, blocks_ref),
        ))
    ]
    for copy in smalls:
        copy.start()

    def up_copies(j):
        columns = pl.ds(pl.multiple_of(j * TILE, TILE), TILE)
        return (
            pltpu.make_async_copy(gate_ref.at[0, :, columns], w_buf.at[j, 0], w_sem.at[j]),
            pltpu.make_async_copy(up_ref.at[0, :, columns], w_buf.at[j, 1], w_sem.at[j]),
        )

    def up_wait(j):
        pltpu.make_async_copy(w_buf.at[j], w_buf.at[j], w_sem.at[j]).wait()

    def down_copies(c):
        slot = lax.rem(up_tiles + c, ring)
        found = []
        for h in range(2):
            columns = pl.ds(pl.multiple_of((2 * c + h) * TILE, TILE), TILE)
            found.append(pltpu.make_async_copy(
                down_ref.at[0, :, columns], w_buf.at[slot, h, pl.ds(0, depth)], w_sem.at[slot]
            ))
        return found

    def down_wait(c):
        slot = lax.rem(up_tiles + c, ring)
        both = w_buf.at[slot, :, pl.ds(0, depth)]
        pltpu.make_async_copy(both, both, w_sem.at[slot]).wait()

    load_states = pltpu.make_async_copy(states_ref, s_all, big_sem.at[0])
    load_cache = pltpu.make_async_copy(kv_ref, c_all, big_sem.at[1])

    @pl.loop(0, EARLY)
    def _(j):
        for copy in up_copies(j):
            copy.start()

    load_states.start()
    load_cache.start()

    @pl.loop(EARLY, up_tiles)
    def _(j):
        for copy in up_copies(j):
            copy.start()

    @pl.loop(0, ring - up_tiles)
    def _(c):
        for copy in down_copies(c):
            copy.start()

    smalls[0].wait()
    smalls[1].wait()
    tok_count = tok_ref.shape[0]
    picks, rows = target_rows(ids_ref, tok_count)
    row_at = lax.broadcasted_iota(jnp.int32, (experts * CAP, tok_count), 0)
    tok_at = lax.broadcasted_iota(jnp.int32, (experts * CAP, tok_count), 1)
    placer = jnp.zeros((experts * CAP, tok_count), jnp.float32)
    for p, row in enumerate(rows):
        placer = jnp.where((row_at == row) & (tok_at == p // 2), 1.0, placer)
    packed = jnp.dot(
        placer.astype(jnp.bfloat16), tok_ref[...], preferred_element_type=jnp.float32
    ).astype(jnp.bfloat16)
    for h in range(PARTS):
        for r in range(experts):
            packed_ref[h, r] = packed[r * CAP : (r + 1) * CAP, h * span : (h + 1) * span]
        x_in[h, e, d] = packed_ref[h, d]

    pl.semaphore_wait(barrier, ranks + 2)

    def pair_of(h, quad, plane):
        return x_in.at[h, quad, pl.ds(plane * 2, 2)]

    def cross(h, quad, plane):
        return pltpu.make_async_remote_copy(
            pair_of(h, quad, plane), pair_of(h, e, plane), cross_send, cross_recv.at[h, plane],
            device_id=(d, across), device_id_type=MESH,
        )

    def to_other(h, quad, plane, where):
        return pltpu.make_async_remote_copy(
            pair_of(h, quad, plane), pair_of(h, quad, plane), pair_send, pair_recv.at[h],
            device_id=(d, where), device_id_type=MESH,
        )

    for h in range(PARTS):
        for i in range(z_count):
            plane = planes(i, True)
            for y in range(2):
                peer = plane * 2 + y

                @pl.when(peer != d)
                def _():
                    pltpu.make_async_remote_copy(
                        packed_ref.at[h, peer], x_in.at[h, e, d], first_send, first_recv.at[h, d // 2],
                        device_id=(peer, e), device_id_type=MESH,
                    ).start()


    smalls[2].wait()
    wide = tok_ref[...].astype(jnp.float32)
    lane = lax.broadcasted_iota(jnp.int32, (tok_count, experts), 1)
    seat = lax.broadcasted_iota(jnp.int32, (tok_count, experts), 0)
    logits = jnp.zeros((tok_count, experts), jnp.float32)
    for r in range(experts):
        product = jnp.sum(wide * router_ref[r : r + 1, :], axis=1, keepdims=True)
        logits = jnp.where(lane == r, product, logits)
    column = lax.broadcasted_iota(jnp.int32, (tok_count, owners * CAP), 1)
    token = lax.broadcasted_iota(jnp.int32, (tok_count, owners * CAP), 0)
    row_of = lax.rem(column, ranks * CAP)
    scores, hits = [], []
    for k in range(2):
        chosen = jnp.zeros(logits.shape, jnp.int32)
        target = jnp.zeros(column.shape, jnp.int32)
        for t in range(tok_count):
            chosen = jnp.where(seat == t, picks[2 * t + k], chosen)
            target = jnp.where(token == t, rows[2 * t + k], target)
        value = jnp.sum(jnp.where(lane == chosen, logits, 0.0), axis=1, keepdims=True)
        scores.append(jax.nn.sigmoid(value))
        hits.append(row_of == target)
    total = scores[0] + scores[1]
    comb = jnp.where(hits[0], scores[0] / total, 0.0) + jnp.where(hits[1], scores[1] / total, 0.0)
    comb_high = comb.astype(jnp.bfloat16)
    comb_low = (comb - comb_high.astype(jnp.float32)).astype(jnp.bfloat16)

    near = [planes(i, False) for i in range(z_count)]

    def relay(h):
        for plane in near:
            cross(h, across, plane).wait_recv()

            @pl.when(core == 1)
            def _():
                to_other(h, across, plane, twin).start()

    for h in range(PARTS):
        for plane in near:
            for count in range(1, 3):

                @pl.when((plane == d // 2) == (count == 1))
                def _():
                    most = x_in.at[h, e, pl.ds(0, count)]
                    pltpu.make_async_copy(most, most, first_recv.at[h, plane]).wait()

            cross(h, e, plane).start()
            to_other(h, e, plane, twin).start()

            @pl.when(core == 0)
            def _():
                to_other(h, e, plane, diagonal).start()

    for copy in smalls[3:]:
        copy.wait()
    load_states.wait()
    load_cache.wait()
    moves = slots_ref.shape[1]
    per_request = blocks_ref.shape[2]
    block_len, lanes = kv_ref.shape[2:]
    pieces = states_ref.shape[2] // lanes
    position = lax.broadcasted_iota(jnp.int32, kv_ref.shape[1:], 1)
    for m in range(moves):
        state = s_all[jnp.maximum(slots_ref[0, m, d], 0)]
        for i in range(pieces):
            pay[0, m, i] = state[:, i * lanes : (i + 1) * lanes]
        for j in range(per_request):
            kept = c_all[jnp.maximum(blocks_ref[m, 0, j, d], 0)].astype(jnp.float32)
            kept = jnp.where(j * block_len + position < len_ref[m, d], kept, 0.0)
            pay[0, m, pl.ds(pieces + 2 * j, 2)] = kept.astype(jnp.bfloat16)
    shifts = []
    for m in range(moves):
        shift = jnp.int32(0)
        for r in range(ranks):
            gap = slots_ref[1, m, r] - r
            gap = gap + jnp.where(gap < 0, ranks, 0)
            shift = jnp.where(slots_ref[1, m, r] >= 0, gap, shift)
        shifts.append(shift)
    bits = ranks.bit_length() - 1

    def bit_of(m, step):
        return 0 if step == bits - 1 else bits - 1 - (step + m) % (bits - 1)

    def hop_copy(m, step):
        bit = 1 << bit_of(m, step)
        peer = d + bit - 2 * bit * lax.rem(d // bit, 2)
        return pltpu.make_async_remote_copy(
            pay.at[step, m], got.at[step, m], mig_send, mig_recv.at[step],
            device_id=(peer, e), device_id_type=MESH,
        )

    def hop_start(step):
        for m in range(moves):
            hop_copy(m, step).start()

    def hop_finish(step):
        pltpu.make_async_copy(got.at[step], got.at[step], mig_recv.at[step]).wait()
        for m in range(moves):
            bit = 1 << bit_of(m, step)
            fixed = sum(1 << bit_of(m, s) for s in range(step + 1))
            loose = ranks - 1 - fixed
            swap = jnp.int32(0)
            for r in range(ranks):
                reach = (r + shifts[m]) & (ranks - 1)
                held = (((d ^ r) & loose) | ((d ^ reach) & fixed)) == 0
                swap = jnp.where(held & (((d ^ r) & bit) != 0), 1, swap)
            pay[step + 1, m] = lax.select(swap > 0, got[step, m], pay[step, m])

    hop_start(0)
    relay(0)

    def gather(h, which):
        for half in range(2):
            at = pl.multiple_of((which * 2 + half) * ranks * CAP, ranks * CAP)
            x_all[pl.ds(at, ranks * CAP), h * span : (h + 1) * span] = jnp.concatenate(
                [x_in[h, half * 2 + which, r] for r in range(ranks)], axis=0
            )

    def pair_wait(h):
        most = x_in.at[h, pl.ds(0, 2)]
        pltpu.make_async_copy(most, most, pair_recv.at[h]).wait()

    gather(0, core)
    pair_wait(0)
    gather(0, 1 - core)

    def product(j, which, h):
        rows_of = pl.ds(h * span, span)
        return jnp.dot(x_all[:, rows_of], w_buf[j, which, rows_of], preferred_element_type=jnp.float32)

    def finish_up(j, gate, upper):
        value = gate / (1.0 + jnp.exp(-gate)) * upper
        hidden[:, j * TILE : (j + 1) * TILE] = value.astype(jnp.bfloat16)

    def refill(j):
        later = j + ring - up_tiles

        if later < down_tiles:
            for copy in down_copies(later):
                copy.start()

    def first_step(tiles):
        for j in tiles:
            up_wait(j)
        for j in tiles:
            for which in range(2):
                part_sum[j, which] = product(j, which, 0)

    def second_step(tiles):
        for j in tiles:
            sums = [part_sum[j, which] for which in range(2)]
            for h in range(1, PARTS):
                sums = [sums[which] + product(j, which, h) for which in range(2)]
            finish_up(j, *sums)
        for j in tiles:
            refill(j)

    def whole_step(tiles):
        for j in tiles:
            up_wait(j)
        for j in tiles:
            gate, upper = [
                jnp.dot(x_all[...], w_buf[j, which], preferred_element_type=jnp.float32)
                for which in range(2)
            ]
            finish_up(j, gate, upper)
        for j in tiles:
            refill(j)

    split = part_sum.shape[0]
    early = split - 2
    first_step(range(early))
    for h in range(1, PARTS):
        relay(h)
        gather(h, core)
    first_step(range(early, split))
    for h in range(1, PARTS):
        pair_wait(h)
        gather(h, 1 - core)
    for start in range(0, split, WIDE):
        second_step(range(start, min(start + WIDE, split)))
        if start == 0:
            hop_finish(0)
            hop_start(1)
    for start in range(split, up_tiles, WIDE):
        whole_step(range(start, min(start + WIDE, up_tiles)))
    wide_count = wide_keep.shape[0]
    groups = [(0, g, 2 * g, 2) for g in range(wide_count)]
    groups += [(1, g, 2 * wide_count + g, 1) for g in range(slim_keep.shape[0])]
    stores = ((wide_keep, wide_pair, wide_home), (slim_keep, slim_pair, slim_home))

    def swap_copy(n):
        kind, g, _, _ = groups[n]
        pair = stores[kind][1]
        return pltpu.make_async_remote_copy(
            pair.at[0, g], pair.at[1, g], half_send, half_recv.at[n],
            device_id=(d, twin), device_id_type=MESH,
        )

    def send_home(n):
        kind, g, _, _ = groups[n]
        keep, pair, home = stores[kind]
        swap_copy(n).wait_recv()
        whole = (keep[g] + pair[1, g]).astype(jnp.bfloat16)
        for o in range(owners):
            home[0, g, o] = whole[o * CAP : (o + 1) * CAP]
        home[1, g, me] = home[0, g, me]

        @pl.loop(1, owners, unroll=True)
        def _(k):
            other = lax.rem(me + k, owners)
            pltpu.make_async_remote_copy(
                home.at[0, g, other], home.at[1, g, me], back_send, back_recv.at[n],
                device_id=(lax.rem(other, ranks), (other // ranks) * 2 + core), device_id_type=MESH,
            ).start()

    def multiply(n):
        kind, g, start, count = groups[n]
        keep, pair, _ = stores[kind]
        for c in range(start, start + count):
            down_wait(c)
        for c in range(start, start + count):
            slot = lax.rem(up_tiles + c, ring)
            for h in range(2):
                part = jnp.dot(
                    hidden[...], w_buf[slot, h, pl.ds(0, depth)], preferred_element_type=jnp.float32
                )
                low, high = part[:rows_half], part[rows_half:]
                first = core == 0
                columns = pl.ds((2 * (c - start) + h) * TILE, TILE)
                keep[g, :, columns] = lax.select(first, low, high)
                pair[0, g, :, columns] = lax.select(first, high, low)
        swap_copy(n).start()

    def mix(n):
        kind, g, start, count = groups[n]
        home = stores[kind][2]
        most = home.at[1, g, pl.ds(0, owners - 1)]
        pltpu.make_async_copy(most, most, back_recv.at[n]).wait()
        rows_in = jnp.concatenate([home[1, g, o] for o in range(owners)], axis=0)
        high = jnp.dot(comb_high, rows_in, preferred_element_type=jnp.float32)
        low = jnp.dot(comb_low, rows_in, preferred_element_type=jnp.float32)
        mixed_ref[:, start * 2 * TILE : (start + count) * 2 * TILE] = (high + low).astype(jnp.bfloat16)

    for n in range(len(groups)):
        multiply(n)
        if n > 0:
            send_home(n - 1)
        else:
            for step in range(1, bits - 1):
                hop_finish(step)
                hop_start(step + 1)
    send_home(len(groups) - 1)
    hop_finish(bits - 1)

    leaving, landing = [], []
    for m in range(moves):
        anchor, arriving = jnp.int32(0), jnp.int32(0)
        for r in range(ranks):
            hit = slots_ref[1, m, r] == d
            anchor = jnp.where(hit, r, anchor)
            arriving = jnp.where(hit, 1, arriving)
        leaving.append((slots_ref[0, m, d], [blocks_ref[m, 0, j, d] for j in range(per_request)]))
        landing.append((
            jnp.where(arriving > 0, slots_ref[2, m, anchor], -1),
            [jnp.where(arriving > 0, blocks_ref[m, 1, j, anchor], -1) for j in range(per_request)],
        ))

    @pl.loop(0, s_all.shape[0])
    def _(s):
        value = s_all[s]
        for m in range(moves):
            value = lax.select(leaving[m][0] == s, jnp.zeros_like(value), value)
        for m in range(moves):
            moved = jnp.concatenate([pay[bits, m, i] for i in range(pieces)], axis=1)
            value = lax.select(landing[m][0] == s, moved, value)
        new_states[s] = value

    @pl.loop(0, c_all.shape[0])
    def _(s):
        value = c_all[s]
        for m in range(moves):
            for j in range(per_request):
                value = lax.select(leaving[m][1][j] == s, jnp.zeros_like(value), value)
        for m in range(moves):
            for j in range(per_request):
                value = lax.select(landing[m][1][j] == s, pay[bits, m, pl.ds(pieces + 2 * j, 2)], value)
        new_cache[s] = value

    for n in range(len(groups)):
        mix(n)

    for step in range(bits):
        pltpu.make_async_copy(pay.at[step], pay.at[step], mig_send).wait()
    most = packed_ref.at[:, pl.ds(0, ranks - 1)]
    pltpu.make_async_copy(most, most, first_send).wait()
    most = x_in.at[:, 0]
    pltpu.make_async_copy(most, most, cross_send).wait()
    most = x_in.at[:, pl.ds(0, 2)]
    pltpu.make_async_copy(most, most, pair_send).wait()
    for _, pair, home in stores:
        pltpu.make_async_copy(pair.at[0], pair.at[0], half_send).wait()
        most = home.at[0, :, pl.ds(0, owners - 1)]
        pltpu.make_async_copy(most, most, back_send).wait()


def fused(
    tokens, router, expert_ids, w_gate, w_up, w_down, states, kv_blocks,
    plan_slots, plan_len, plan_blocks,
):
    ranks, quads = lax.axis_size("dp"), lax.axis_size("ep")
    experts = router.shape[1]
    tok_count, width = tokens.shape
    moves = plan_slots.shape[1]
    per_request = plan_blocks.shape[3]
    bf16 = jnp.bfloat16
    dma = pltpu.SemaphoreType.DMA
    like = jax.ShapeDtypeStruct
    ids = expert_ids.T
    slots = jnp.transpose(plan_slots, (2, 1, 0))
    lengths = plan_len.T
    blocks = jnp.transpose(plan_blocks, (1, 2, 3, 0))
    routes = router.T
    depth = w_gate.shape[2]
    down_tiles = width // (2 * TILE)
    owners = 2 * ranks
    bits = ranks.bit_length() - 1
    slim = 2 + down_tiles % 2
    wide = (down_tiles - slim) // 2
    lanes = kv_blocks.shape[3]
    request = (states.shape[2] // lanes + per_request * kv_blocks.shape[1], *kv_blocks.shape[2:])
    outputs = pl.pallas_call(
        functools.partial(expert_kernel, ranks, quads),
        out_shape=(
            pltpu.VMEM(states.shape, bf16),
            pltpu.VMEM(kv_blocks.shape, bf16),
            pltpu.VMEM(tokens.shape, bf16),
        ),
        in_specs=[ANY] * 11,
        out_specs=(VMEM, VMEM, VMEM),
        scratch_shapes=[
            pltpu.SMEM(ids.shape, jnp.int32),
            pltpu.SMEM(slots.shape, jnp.int32),
            pltpu.SMEM(lengths.shape, jnp.int32),
            pltpu.SMEM(blocks.shape, jnp.int32),
            pltpu.VMEM(tokens.shape, bf16),
            pltpu.VMEM(routes.shape, jnp.float32),
            pltpu.VMEM((PARTS, experts, CAP, width // PARTS), bf16),
            pltpu.VMEM(states.shape, bf16),
            pltpu.VMEM(kv_blocks.shape, bf16),
            pltpu.VMEM((bits + 1, moves, *request), bf16),
            pltpu.VMEM((bits, moves, *request), bf16),
            pltpu.VMEM((RING, 2, width, TILE), bf16),
            pltpu.VMEM((PARTS, quads, ranks, CAP, width // PARTS), bf16),
            pltpu.VMEM((quads * ranks * CAP, width), bf16),
            pltpu.VMEM((SPLIT, 2, quads * ranks * CAP, TILE), jnp.float32),
            pltpu.VMEM((quads * ranks * CAP, depth), bf16),
            *[
                spec
                for count, columns in ((wide, 4 * TILE), (slim, 2 * TILE))
                for spec in (
                    pltpu.VMEM((count, owners * CAP, columns), jnp.float32),
                    pltpu.VMEM((2, count, owners * CAP, columns), jnp.float32),
                    pltpu.VMEM((2, count, owners, CAP, columns), bf16),
                )
            ],
            dma((6,)), dma((2,)), dma((RING,)), dma, dma((PARTS, ranks // 2)), dma, dma((PARTS, ranks // 2)),
            dma, dma((PARTS,)),
            dma, dma((wide + slim,)), dma, dma((wide + slim,)), dma, dma((bits,)),
        ],
        compiler_params=pltpu.CompilerParams(
            collective_id=0, has_side_effects=True, vmem_limit_bytes=VMEM_LIMIT
        ),
        name="expert",
    )(
        ids, slots, lengths, blocks, tokens, routes, w_gate, w_up, w_down, states, kv_blocks
    )
    outputs = [pltpu.with_memory_space_constraint(o, pltpu.VMEM) for o in outputs]
    new_states, new_cache, mixed = pl.pallas_call(
        land_kernel,
        out_shape=(like(states.shape, bf16), like(kv_blocks.shape, bf16), like(tokens.shape, bf16)),
        in_specs=[VMEM] * 3,
        out_specs=(ANY, ANY, ANY),
        scratch_shapes=[dma((3,))],
        compiler_params=pltpu.CompilerParams(vmem_limit_bytes=LAND_LIMIT),
        name="land",
    )(*outputs)
    return mixed, new_states, new_cache


def local(
    tokens,
    router,
    expert_ids,
    w_gate,
    w_up,
    w_down,
    states,
    kv_blocks,
    plan_slots,
    plan_len,
    plan_blocks,
):
    ranks = lax.axis_size("dp")
    here = lax.axis_index("dp")
    moves = plan_slots.shape[1]
    slot_count = states.shape[0]
    block_count = kv_blocks.shape[0]
    per_request = plan_blocks.shape[3]
    block_len = kv_blocks.shape[2]
    mine = lax.dynamic_index_in_dim(plan_slots, here, 0, keepdims=False)
    my_blocks = lax.dynamic_index_in_dim(plan_blocks, here, 0, keepdims=False)
    my_length = lax.dynamic_index_in_dim(plan_len, here, 0, keepdims=False)
    leaving_slot = mine[:, 0]
    leaving_block = my_blocks[:, 0, :]
    state_out = states[jnp.maximum(leaving_slot, 0)]
    state_out = jnp.where((leaving_slot >= 0)[:, None, None], state_out, jnp.zeros_like(state_out))
    cache_out = kv_blocks[jnp.maximum(leaving_block, 0)]
    position = jnp.arange(per_request)[:, None] * block_len + jnp.arange(block_len)[None, :]
    written = (leaving_block >= 0)[:, :, None] & (position[None] < my_length[:, None, None])
    cache_out = jnp.where(written[:, :, None, :, None], cache_out, jnp.zeros_like(cache_out))
    arrivals = plan_slots[:, :, 1] == here
    sender = jnp.sum(jnp.where(arrivals, jnp.arange(ranks)[:, None], 0), axis=0)
    arriving = jnp.any(arrivals, axis=0)
    peers = jnp.arange(ranks)
    match = mine[:, 1][None, :] == peers[:, None]
    which = jnp.sum(jnp.where(match, jnp.arange(moves)[None, :], 0), axis=1)
    filled = jnp.any(match, axis=1)
    send_state = jnp.where(
        filled[:, None, None], state_out[which], jnp.zeros_like(state_out[which])
    )
    send_cache = jnp.where(
        filled[:, None, None, None, None], cache_out[which], jnp.zeros_like(cache_out[which])
    )
    got_state, got_cache = (
        lax.all_to_all(send_state, "dp", split_axis=0, concat_axis=0, tiled=True),
        lax.all_to_all(send_cache, "dp", split_axis=0, concat_axis=0, tiled=True),
    )
    state_in = got_state[sender]
    cache_in = got_cache[sender]
    slot_line = jnp.arange(slot_count)
    gone = jnp.any(slot_line[:, None] == leaving_slot[None, :], axis=1)
    new_states = jnp.where(gone[:, None, None], jnp.zeros_like(states), states)
    block_line = jnp.arange(block_count)
    gone_blocks = jnp.any(block_line[:, None, None] == leaving_block[None], axis=(1, 2))
    new_cache = jnp.where(gone_blocks[:, None, None, None], jnp.zeros_like(kv_blocks), kv_blocks)
    for move_index in range(moves):
        anchor = sender[move_index]
        place = plan_slots[anchor, move_index, 2]
        landing = (slot_line == place) & arriving[move_index]
        new_states = jnp.where(landing[:, None, None], state_in[move_index][None], new_states)
        for block_index in range(per_request):
            spot = plan_blocks[anchor, move_index, 1, block_index]
            block_hit = (block_line == spot) & arriving[move_index]
            new_cache = jnp.where(
                block_hit[:, None, None, None], cache_in[move_index, block_index][None], new_cache
            )
    experts = router.shape[1]
    tok_count = tokens.shape[0]
    width = tokens.shape[1]
    group = ranks // experts
    flat_ids = expert_ids.reshape(-1)
    onehot = (flat_ids[:, None] == jnp.arange(experts)[None, :]).astype(jnp.int32)
    earlier = jnp.cumsum(onehot, axis=0) - onehot
    slot_of = jnp.sum(earlier * onehot, axis=1)
    target_row = flat_ids * CAP + slot_of
    placer = (jnp.arange(experts * CAP)[:, None] == target_row[None, :]).astype(jnp.bfloat16)
    doubled = jnp.repeat(tokens, 2, axis=0)
    packed = jnp.dot(placer, doubled, preferred_element_type=jnp.float32).astype(jnp.bfloat16)
    outgoing = jnp.repeat(packed.reshape(experts, CAP, width), group, axis=0)
    incoming = lax.all_to_all(outgoing, "dp", split_axis=0, concat_axis=0, tiled=True)
    rows_in = incoming.reshape(ranks * CAP, width)
    piece = lax.all_gather(rows_in, "ep", axis=0, tiled=True)
    gate = jnp.dot(piece, w_gate[0], preferred_element_type=jnp.float32)
    upper = jnp.dot(piece, w_up[0], preferred_element_type=jnp.float32)
    hidden = (jax.nn.silu(gate) * upper).astype(jnp.bfloat16)
    summed = lax.psum_scatter(
        jnp.dot(hidden, w_down[0], preferred_element_type=jnp.float32),
        "ep",
        scatter_dimension=0,
        tiled=True,
    )
    returned = lax.all_to_all(
        summed.reshape(ranks, CAP, width), "dp", split_axis=0, concat_axis=0, tiled=True
    )
    expert_out = jnp.sum(returned.reshape(experts, group, CAP, width), axis=1).reshape(
        experts * CAP, width
    )
    chosen = expert_out[target_row].reshape(tok_count, 2, width)
    logits = jnp.dot(tokens.astype(jnp.float32), router, precision=lax.Precision.HIGHEST)
    scores = jax.nn.sigmoid(jnp.take_along_axis(logits, expert_ids, axis=1))
    weights = scores / jnp.sum(scores, axis=1, keepdims=True)
    mixed = jnp.sum(weights[:, :, None] * chosen, axis=1).astype(jnp.bfloat16)
    return (mixed, new_states, new_cache)


def solution(mesh):
    placed = (
        P(("dp", "ep"), None),
        P(),
        P(("dp", "ep"), None),
        P("dp", None, "ep"),
        P("dp", None, "ep"),
        P("dp", "ep", None),
        P("dp", None, "ep"),
        P("dp", None, None, "ep"),
        P(),
        P(),
        P(),
    )
    def step(*args):
        ranks, quads = lax.axis_size("dp"), lax.axis_size("ep")
        one_slab = args[1].shape[1] == ranks and ranks & (ranks - 1) == 0
        two_by_two = quads == 2 * 2
        return (fused if one_slab and two_by_two else local)(*args)

    return jax.shard_map(
        step,
        mesh=mesh,
        in_specs=placed,
        out_specs=(P(("dp", "ep"), None), P("dp", None, "ep"), P("dp", None, None, "ep")),
        check_vma=False,
    )
```

```python
import functools

import jax
import jax.numpy as jnp
from jax import lax
from jax.experimental import pallas as pl
from jax.experimental.pallas import tpu as pltpu
from jax.sharding import PartitionSpec as P

CAP = 2
MESH = pl.DeviceIdType.MESH
ANY = pl.BlockSpec(memory_space=pl.ANY)
VMEM = pl.BlockSpec(memory_space=pltpu.VMEM)
SMEM = pl.BlockSpec(memory_space=pltpu.SMEM)
VMEM_LIMIT = 65_000_000
TILE = 256
RING = 13
EARLY = 2
WIDE = 3
PARTS = 2
SPLIT = 6
LAND_LIMIT = 1 << 20


def target_rows(ids_ref, tok_count):
    picks = [ids_ref[k, t] for t in range(tok_count) for k in range(2)]
    rows = []
    for p, expert in enumerate(picks):
        slot = jnp.int32(0)
        for q in range(p):
            slot = slot + jnp.where(picks[q] == expert, 1, 0)
        rows.append(expert * CAP + slot)
    return picks, rows


def land_kernel(states_ref, cache_ref, mixed_ref, new_states, new_cache, new_mixed, sem):
    pairs = ((states_ref, new_states), (cache_ref, new_cache), (mixed_ref, new_mixed))
    copies = [pltpu.make_async_copy(a, b, sem.at[i]) for i, (a, b) in enumerate(pairs)]
    for copy in copies:
        copy.start()
    for copy in copies:
        copy.wait()


def expert_kernel(
    ranks, quads,
    ids_hbm, slots_hbm, len_hbm, blocks_hbm, tok_hbm, router_hbm, gate_ref, up_ref, down_ref,
    states_ref, kv_ref,
    new_states, new_cache, mixed_ref,
    ids_ref, slots_ref, len_ref, blocks_ref, tok_ref, router_ref,
    packed_ref, s_all, c_all, pay, got,
    w_buf, x_in, x_all, part_sum, hidden, wide_keep, wide_pair, wide_home, slim_keep, slim_pair, slim_home,
    small_sem, big_sem, w_sem, first_send, first_recv, cross_send, cross_recv, pair_send, pair_recv,
    half_send, half_recv, back_send, back_recv, mig_send, mig_recv,
):
    d = lax.axis_index("dp")
    e = lax.axis_index("ep")
    side, core = e // 2, lax.rem(e, 2)
    across, twin = (1 - side) * 2 + core, side * 2 + 1 - core
    diagonal = (1 - side) * 2 + 1 - core
    experts = ranks
    up_tiles = gate_ref.shape[2] // TILE
    down_tiles = down_ref.shape[2] // (2 * TILE)
    depth = down_ref.shape[1]
    ring = w_buf.shape[0]
    rows_half = 2 * ranks * CAP
    owners = 2 * ranks
    span = packed_ref.shape[3]
    me = side * ranks + d

    barrier = pltpu.get_barrier_semaphore()

    z_count = ranks // 2

    def planes(i, reverse):
        forward = (d // 2 < z_count // 2) == (not reverse)
        return jnp.where(forward, i, z_count - 1 - i)

    for i in range(z_count):
        for flip in range(2):
            other = planes(i, True) * 2 + lax.rem(d + 1 + flip, 2)

            @pl.when(other != d)
            def _():
                pl.semaphore_signal(barrier, inc=1, device_id=(other, e), device_id_type=MESH)

    for quad in (across, diagonal, twin):
        pl.semaphore_signal(barrier, inc=1, device_id=(d, quad), device_id_type=MESH)

    smalls = [
        pltpu.make_async_copy(a, b, small_sem.at[i])
        for i, (a, b) in enumerate((
            (tok_hbm, tok_ref), (ids_hbm, ids_ref), (router_hbm, router_ref),
            (slots_hbm, slots_ref), (len_hbm, len_ref), (blocks_hbm, blocks_ref),
        ))
    ]
    for copy in smalls:
        copy.start()

    def up_copies(j):
        columns = pl.ds(pl.multiple_of(j * TILE, TILE), TILE)
        return (
            pltpu.make_async_copy(gate_ref.at[0, :, columns], w_buf.at[j, 0], w_sem.at[j]),
            pltpu.make_async_copy(up_ref.at[0, :, columns], w_buf.at[j, 1], w_sem.at[j]),
        )

    def up_wait(j):
        pltpu.make_async_copy(w_buf.at[j], w_buf.at[j], w_sem.at[j]).wait()

    def down_copies(c):
        slot = lax.rem(up_tiles + c, ring)
        found = []
        for h in range(2):
            columns = pl.ds(pl.multiple_of((2 * c + h) * TILE, TILE), TILE)
            found.append(pltpu.make_async_copy(
                down_ref.at[0, :, columns], w_buf.at[slot, h, pl.ds(0, depth)], w_sem.at[slot]
            ))
        return found

    def down_wait(c):
        slot = lax.rem(up_tiles + c, ring)
        both = w_buf.at[slot, :, pl.ds(0, depth)]
        pltpu.make_async_copy(both, both, w_sem.at[slot]).wait()

    load_states = pltpu.make_async_copy(states_ref, s_all, big_sem.at[0])
    load_cache = pltpu.make_async_copy(kv_ref, c_all, big_sem.at[1])

    @pl.loop(0, EARLY)
    def _(j):
        for copy in up_copies(j):
            copy.start()

    load_states.start()
    load_cache.start()

    @pl.loop(EARLY, up_tiles)
    def _(j):
        for copy in up_copies(j):
            copy.start()

    @pl.loop(0, ring - up_tiles)
    def _(c):
        for copy in down_copies(c):
            copy.start()

    smalls[0].wait()
    smalls[1].wait()
    tok_count = tok_ref.shape[0]
    picks, rows = target_rows(ids_ref, tok_count)
    row_at = lax.broadcasted_iota(jnp.int32, (experts * CAP, tok_count), 0)
    tok_at = lax.broadcasted_iota(jnp.int32, (experts * CAP, tok_count), 1)
    placer = jnp.zeros((experts * CAP, tok_count), jnp.float32)
    for p, row in enumerate(rows):
        placer = jnp.where((row_at == row) & (tok_at == p // 2), 1.0, placer)
    packed = jnp.dot(
        placer.astype(jnp.bfloat16), tok_ref[...], preferred_element_type=jnp.float32
    ).astype(jnp.bfloat16)
    for h in range(PARTS):
        for r in range(experts):
            packed_ref[h, r] = packed[r * CAP : (r + 1) * CAP, h * span : (h + 1) * span]
        x_in[h, e, d] = packed_ref[h, d]

    pl.semaphore_wait(barrier, ranks + 2)

    def pair_of(h, quad, plane):
        return x_in.at[h, quad, pl.ds(plane * 2, 2)]

    def cross(h, quad, plane):
        return pltpu.make_async_remote_copy(
            pair_of(h, quad, plane), pair_of(h, e, plane), cross_send, cross_recv.at[h, plane],
            device_id=(d, across), device_id_type=MESH,
        )

    def to_other(h, quad, plane, where):
        return pltpu.make_async_remote_copy(
            pair_of(h, quad, plane), pair_of(h, quad, plane), pair_send, pair_recv.at[h],
            device_id=(d, where), device_id_type=MESH,
        )

    for h in range(PARTS):
        for i in range(z_count):
            plane = planes(i, True)
            for y in range(2):
                peer = plane * 2 + y

                @pl.when(peer != d)
                def _():
                    pltpu.make_async_remote_copy(
                        packed_ref.at[h, peer], x_in.at[h, e, d], first_send, first_recv.at[h, d // 2],
                        device_id=(peer, e), device_id_type=MESH,
                    ).start()


    smalls[2].wait()
    wide = tok_ref[...].astype(jnp.float32)
    lane = lax.broadcasted_iota(jnp.int32, (tok_count, experts), 1)
    seat = lax.broadcasted_iota(jnp.int32, (tok_count, experts), 0)
    logits = jnp.zeros((tok_count, experts), jnp.float32)
    for r in range(experts):
        product = jnp.sum(wide * router_ref[r : r + 1, :], axis=1, keepdims=True)
        logits = jnp.where(lane == r, product, logits)
    column = lax.broadcasted_iota(jnp.int32, (tok_count, owners * CAP), 1)
    token = lax.broadcasted_iota(jnp.int32, (tok_count, owners * CAP), 0)
    row_of = lax.rem(column, ranks * CAP)
    scores, hits = [], []
    for k in range(2):
        chosen = jnp.zeros(logits.shape, jnp.int32)
        target = jnp.zeros(column.shape, jnp.int32)
        for t in range(tok_count):
            chosen = jnp.where(seat == t, picks[2 * t + k], chosen)
            target = jnp.where(token == t, rows[2 * t + k], target)
        value = jnp.sum(jnp.where(lane == chosen, logits, 0.0), axis=1, keepdims=True)
        scores.append(jax.nn.sigmoid(value))
        hits.append(row_of == target)
    total = scores[0] + scores[1]
    comb = jnp.where(hits[0], scores[0] / total, 0.0) + jnp.where(hits[1], scores[1] / total, 0.0)
    comb_high = comb.astype(jnp.bfloat16)
    comb_low = (comb - comb_high.astype(jnp.float32)).astype(jnp.bfloat16)

    near = [planes(i, False) for i in range(z_count)]

    def relay(h):
        for plane in near:
            cross(h, across, plane).wait_recv()

            @pl.when(core == 1)
            def _():
                to_other(h, across, plane, twin).start()

    for h in range(PARTS):
        for plane in near:
            for count in range(1, 3):

                @pl.when((plane == d // 2) == (count == 1))
                def _():
                    most = x_in.at[h, e, pl.ds(0, count)]
                    pltpu.make_async_copy(most, most, first_recv.at[h, plane]).wait()

            cross(h, e, plane).start()
            to_other(h, e, plane, twin).start()

            @pl.when(core == 0)
            def _():
                to_other(h, e, plane, diagonal).start()

    for copy in smalls[3:]:
        copy.wait()
    load_states.wait()
    load_cache.wait()
    moves = slots_ref.shape[1]
    per_request = blocks_ref.shape[2]
    block_len, lanes = kv_ref.shape[2:]
    pieces = states_ref.shape[2] // lanes
    position = lax.broadcasted_iota(jnp.int32, kv_ref.shape[1:], 1)
    for m in range(moves):
        state = s_all[jnp.maximum(slots_ref[0, m, d], 0)]
        for i in range(pieces):
            pay[0, m, i] = state[:, i * lanes : (i + 1) * lanes]
        for j in range(per_request):
            kept = c_all[jnp.maximum(blocks_ref[m, 0, j, d], 0)].astype(jnp.float32)
            kept = jnp.where(j * block_len + position < len_ref[m, d], kept, 0.0)
            pay[0, m, pl.ds(pieces + 2 * j, 2)] = kept.astype(jnp.bfloat16)
    shifts = []
    for m in range(moves):
        shift = jnp.int32(0)
        for r in range(ranks):
            gap = slots_ref[1, m, r] - r
            gap = gap + jnp.where(gap < 0, ranks, 0)
            shift = jnp.where(slots_ref[1, m, r] >= 0, gap, shift)
        shifts.append(shift)
    bits = ranks.bit_length() - 1

    def bit_of(m, step):
        return 0 if step == bits - 1 else bits - 1 - (step + m) % (bits - 1)

    def hop_copy(m, step):
        bit = 1 << bit_of(m, step)
        peer = d + bit - 2 * bit * lax.rem(d // bit, 2)
        return pltpu.make_async_remote_copy(
            pay.at[step, m], got.at[step, m], mig_send, mig_recv.at[step],
            device_id=(peer, e), device_id_type=MESH,
        )

    def hop_start(step):
        for m in range(moves):
            hop_copy(m, step).start()

    def hop_finish(step):
        pltpu.make_async_copy(got.at[step], got.at[step], mig_recv.at[step]).wait()
        for m in range(moves):
            bit = 1 << bit_of(m, step)
            fixed = sum(1 << bit_of(m, s) for s in range(step + 1))
            loose = ranks - 1 - fixed
            swap = jnp.int32(0)
            for r in range(ranks):
                reach = (r + shifts[m]) & (ranks - 1)
                held = (((d ^ r) & loose) | ((d ^ reach) & fixed)) == 0
                swap = jnp.where(held & (((d ^ r) & bit) != 0), 1, swap)
            pay[step + 1, m] = lax.select(swap > 0, got[step, m], pay[step, m])

    hop_start(0)
    relay(0)

    def gather(h, which):
        for half in range(2):
            at = pl.multiple_of((which * 2 + half) * ranks * CAP, ranks * CAP)
            x_all[pl.ds(at, ranks * CAP), h * span : (h + 1) * span] = jnp.concatenate(
                [x_in[h, half * 2 + which, r] for r in range(ranks)], axis=0
            )

    def pair_wait(h):
        most = x_in.at[h, pl.ds(0, 2)]
        pltpu.make_async_copy(most, most, pair_recv.at[h]).wait()

    gather(0, core)
    pair_wait(0)
    gather(0, 1 - core)

    def product(j, which, h):
        rows_of = pl.ds(h * span, span)
        return jnp.dot(x_all[:, rows_of], w_buf[j, which, rows_of], preferred_element_type=jnp.float32)

    def finish_up(j, gate, upper):
        value = gate / (1.0 + jnp.exp(-gate)) * upper
        hidden[:, j * TILE : (j + 1) * TILE] = value.astype(jnp.bfloat16)

    def refill(j):
        later = j + ring - up_tiles

        if later < down_tiles:
            for copy in down_copies(later):
                copy.start()

    def first_step(tiles):
        for j in tiles:
            up_wait(j)
        for j in tiles:
            for which in range(2):
                part_sum[j, which] = product(j, which, 0)

    def second_step(tiles):
        for j in tiles:
            sums = [part_sum[j, which] for which in range(2)]
            for h in range(1, PARTS):
                sums = [sums[which] + product(j, which, h) for which in range(2)]
            finish_up(j, *sums)
        for j in tiles:
            refill(j)

    def whole_step(tiles):
        for j in tiles:
            up_wait(j)
        for j in tiles:
            gate, upper = [
                jnp.dot(x_all[...], w_buf[j, which], preferred_element_type=jnp.float32)
                for which in range(2)
            ]
            finish_up(j, gate, upper)
        for j in tiles:
            refill(j)

    split = part_sum.shape[0]
    early = split - 2
    first_step(range(early))
    for h in range(1, PARTS):
        relay(h)
        gather(h, core)
    first_step(range(early, split))
    for h in range(1, PARTS):
        pair_wait(h)
        gather(h, 1 - core)
    for start in range(0, split, WIDE):
        second_step(range(start, min(start + WIDE, split)))
        if start == 0:
            hop_finish(0)
            hop_start(1)
    for start in range(split, up_tiles, WIDE):
        whole_step(range(start, min(start + WIDE, up_tiles)))
    wide_count = wide_keep.shape[0]
    groups = [(0, g, 2 * g, 2) for g in range(wide_count)]
    groups += [(1, g, 2 * wide_count + g, 1) for g in range(slim_keep.shape[0])]
    stores = ((wide_keep, wide_pair, wide_home), (slim_keep, slim_pair, slim_home))

    def swap_copy(n):
        kind, g, _, _ = groups[n]
        pair = stores[kind][1]
        return pltpu.make_async_remote_copy(
            pair.at[0, g], pair.at[1, g], half_send, half_recv.at[n],
            device_id=(d, twin), device_id_type=MESH,
        )

    def send_home(n):
        kind, g, _, _ = groups[n]
        keep, pair, home = stores[kind]
        swap_copy(n).wait_recv()
        whole = (keep[g] + pair[1, g].astype(jnp.float32)).astype(jnp.bfloat16)
        for o in range(owners):
            home[0, g, o] = whole[o * CAP : (o + 1) * CAP]
        home[1, g, me] = home[0, g, me]

        @pl.loop(1, owners, unroll=True)
        def _(k):
            other = lax.rem(me + k, owners)
            pltpu.make_async_remote_copy(
                home.at[0, g, other], home.at[1, g, me], back_send, back_recv.at[n],
                device_id=(lax.rem(other, ranks), (other // ranks) * 2 + core), device_id_type=MESH,
            ).start()

    def multiply(n):
        kind, g, start, count = groups[n]
        keep, pair, _ = stores[kind]
        for c in range(start, start + count):
            down_wait(c)
        for c in range(start, start + count):
            slot = lax.rem(up_tiles + c, ring)
            for h in range(2):
                part = jnp.dot(
                    hidden[...], w_buf[slot, h, pl.ds(0, depth)], preferred_element_type=jnp.float32
                )
                low, high = part[:rows_half], part[rows_half:]
                first = core == 0
                columns = pl.ds((2 * (c - start) + h) * TILE, TILE)
                keep[g, :, columns] = lax.select(first, low, high)
                pair[0, g, :, columns] = lax.select(first, high, low).astype(jnp.bfloat16)
        swap_copy(n).start()

    def mix(n):
        kind, g, start, count = groups[n]
        home = stores[kind][2]
        most = home.at[1, g, pl.ds(0, owners - 1)]
        pltpu.make_async_copy(most, most, back_recv.at[n]).wait()
        rows_in = jnp.concatenate([home[1, g, o] for o in range(owners)], axis=0)
        high = jnp.dot(comb_high, rows_in, preferred_element_type=jnp.float32)
        low = jnp.dot(comb_low, rows_in, preferred_element_type=jnp.float32)
        mixed_ref[:, start * 2 * TILE : (start + count) * 2 * TILE] = (high + low).astype(jnp.bfloat16)

    for n in range(len(groups)):
        multiply(n)
        if n > 0:
            send_home(n - 1)
        else:
            for step in range(1, bits - 1):
                hop_finish(step)
                hop_start(step + 1)
    send_home(len(groups) - 1)
    hop_finish(bits - 1)

    leaving, landing = [], []
    for m in range(moves):
        anchor, arriving = jnp.int32(0), jnp.int32(0)
        for r in range(ranks):
            hit = slots_ref[1, m, r] == d
            anchor = jnp.where(hit, r, anchor)
            arriving = jnp.where(hit, 1, arriving)
        leaving.append((slots_ref[0, m, d], [blocks_ref[m, 0, j, d] for j in range(per_request)]))
        landing.append((
            jnp.where(arriving > 0, slots_ref[2, m, anchor], -1),
            [jnp.where(arriving > 0, blocks_ref[m, 1, j, anchor], -1) for j in range(per_request)],
        ))

    @pl.loop(0, s_all.shape[0])
    def _(s):
        value = s_all[s]
        for m in range(moves):
            value = lax.select(leaving[m][0] == s, jnp.zeros_like(value), value)
        for m in range(moves):
            moved = jnp.concatenate([pay[bits, m, i] for i in range(pieces)], axis=1)
            value = lax.select(landing[m][0] == s, moved, value)
        new_states[s] = value

    @pl.loop(0, c_all.shape[0])
    def _(s):
        value = c_all[s]
        for m in range(moves):
            for j in range(per_request):
                value = lax.select(leaving[m][1][j] == s, jnp.zeros_like(value), value)
        for m in range(moves):
            for j in range(per_request):
                value = lax.select(landing[m][1][j] == s, pay[bits, m, pl.ds(pieces + 2 * j, 2)], value)
        new_cache[s] = value

    for n in range(len(groups)):
        mix(n)

    for step in range(bits):
        pltpu.make_async_copy(pay.at[step], pay.at[step], mig_send).wait()
    most = packed_ref.at[:, pl.ds(0, ranks - 1)]
    pltpu.make_async_copy(most, most, first_send).wait()
    most = x_in.at[:, 0]
    pltpu.make_async_copy(most, most, cross_send).wait()
    most = x_in.at[:, pl.ds(0, 2)]
    pltpu.make_async_copy(most, most, pair_send).wait()
    for _, pair, home in stores:
        pltpu.make_async_copy(pair.at[0], pair.at[0], half_send).wait()
        most = home.at[0, :, pl.ds(0, owners - 1)]
        pltpu.make_async_copy(most, most, back_send).wait()


def fused(
    tokens, router, expert_ids, w_gate, w_up, w_down, states, kv_blocks,
    plan_slots, plan_len, plan_blocks,
):
    ranks, quads = lax.axis_size("dp"), lax.axis_size("ep")
    experts = router.shape[1]
    tok_count, width = tokens.shape
    moves = plan_slots.shape[1]
    per_request = plan_blocks.shape[3]
    bf16 = jnp.bfloat16
    dma = pltpu.SemaphoreType.DMA
    like = jax.ShapeDtypeStruct
    ids = expert_ids.T
    slots = jnp.transpose(plan_slots, (2, 1, 0))
    lengths = plan_len.T
    blocks = jnp.transpose(plan_blocks, (1, 2, 3, 0))
    routes = router.T
    depth = w_gate.shape[2]
    down_tiles = width // (2 * TILE)
    owners = 2 * ranks
    bits = ranks.bit_length() - 1
    slim = 2 + down_tiles % 2
    wide = (down_tiles - slim) // 2
    lanes = kv_blocks.shape[3]
    request = (states.shape[2] // lanes + per_request * kv_blocks.shape[1], *kv_blocks.shape[2:])
    outputs = pl.pallas_call(
        functools.partial(expert_kernel, ranks, quads),
        out_shape=(
            pltpu.VMEM(states.shape, bf16),
            pltpu.VMEM(kv_blocks.shape, bf16),
            pltpu.VMEM(tokens.shape, bf16),
        ),
        in_specs=[ANY] * 11,
        out_specs=(VMEM, VMEM, VMEM),
        scratch_shapes=[
            pltpu.SMEM(ids.shape, jnp.int32),
            pltpu.SMEM(slots.shape, jnp.int32),
            pltpu.SMEM(lengths.shape, jnp.int32),
            pltpu.SMEM(blocks.shape, jnp.int32),
            pltpu.VMEM(tokens.shape, bf16),
            pltpu.VMEM(routes.shape, jnp.float32),
            pltpu.VMEM((PARTS, experts, CAP, width // PARTS), bf16),
            pltpu.VMEM(states.shape, bf16),
            pltpu.VMEM(kv_blocks.shape, bf16),
            pltpu.VMEM((bits + 1, moves, *request), bf16),
            pltpu.VMEM((bits, moves, *request), bf16),
            pltpu.VMEM((RING, 2, width, TILE), bf16),
            pltpu.VMEM((PARTS, quads, ranks, CAP, width // PARTS), bf16),
            pltpu.VMEM((quads * ranks * CAP, width), bf16),
            pltpu.VMEM((SPLIT, 2, quads * ranks * CAP, TILE), jnp.float32),
            pltpu.VMEM((quads * ranks * CAP, depth), bf16),
            *[
                spec
                for count, columns in ((wide, 4 * TILE), (slim, 2 * TILE))
                for spec in (
                    pltpu.VMEM((count, owners * CAP, columns), jnp.float32),
                    pltpu.VMEM((2, count, owners * CAP, columns), bf16),
                    pltpu.VMEM((2, count, owners, CAP, columns), bf16),
                )
            ],
            dma((6,)), dma((2,)), dma((RING,)), dma, dma((PARTS, ranks // 2)), dma, dma((PARTS, ranks // 2)),
            dma, dma((PARTS,)),
            dma, dma((wide + slim,)), dma, dma((wide + slim,)), dma, dma((bits,)),
        ],
        compiler_params=pltpu.CompilerParams(
            collective_id=0, has_side_effects=True, vmem_limit_bytes=VMEM_LIMIT
        ),
        name="expert",
    )(
        ids, slots, lengths, blocks, tokens, routes, w_gate, w_up, w_down, states, kv_blocks
    )
    outputs = [pltpu.with_memory_space_constraint(o, pltpu.VMEM) for o in outputs]
    new_states, new_cache, mixed = pl.pallas_call(
        land_kernel,
        out_shape=(like(states.shape, bf16), like(kv_blocks.shape, bf16), like(tokens.shape, bf16)),
        in_specs=[VMEM] * 3,
        out_specs=(ANY, ANY, ANY),
        scratch_shapes=[dma((3,))],
        compiler_params=pltpu.CompilerParams(vmem_limit_bytes=LAND_LIMIT),
        name="land",
    )(*outputs)
    return mixed, new_states, new_cache


def local(
    tokens,
    router,
    expert_ids,
    w_gate,
    w_up,
    w_down,
    states,
    kv_blocks,
    plan_slots,
    plan_len,
    plan_blocks,
):
    ranks = lax.axis_size("dp")
    here = lax.axis_index("dp")
    moves = plan_slots.shape[1]
    slot_count = states.shape[0]
    block_count = kv_blocks.shape[0]
    per_request = plan_blocks.shape[3]
    block_len = kv_blocks.shape[2]
    mine = lax.dynamic_index_in_dim(plan_slots, here, 0, keepdims=False)
    my_blocks = lax.dynamic_index_in_dim(plan_blocks, here, 0, keepdims=False)
    my_length = lax.dynamic_index_in_dim(plan_len, here, 0, keepdims=False)
    leaving_slot = mine[:, 0]
    leaving_block = my_blocks[:, 0, :]
    state_out = states[jnp.maximum(leaving_slot, 0)]
    state_out = jnp.where((leaving_slot >= 0)[:, None, None], state_out, jnp.zeros_like(state_out))
    cache_out = kv_blocks[jnp.maximum(leaving_block, 0)]
    position = jnp.arange(per_request)[:, None] * block_len + jnp.arange(block_len)[None, :]
    written = (leaving_block >= 0)[:, :, None] & (position[None] < my_length[:, None, None])
    cache_out = jnp.where(written[:, :, None, :, None], cache_out, jnp.zeros_like(cache_out))
    arrivals = plan_slots[:, :, 1] == here
    sender = jnp.sum(jnp.where(arrivals, jnp.arange(ranks)[:, None], 0), axis=0)
    arriving = jnp.any(arrivals, axis=0)
    peers = jnp.arange(ranks)
    match = mine[:, 1][None, :] == peers[:, None]
    which = jnp.sum(jnp.where(match, jnp.arange(moves)[None, :], 0), axis=1)
    filled = jnp.any(match, axis=1)
    send_state = jnp.where(
        filled[:, None, None], state_out[which], jnp.zeros_like(state_out[which])
    )
    send_cache = jnp.where(
        filled[:, None, None, None, None], cache_out[which], jnp.zeros_like(cache_out[which])
    )
    got_state, got_cache = (
        lax.all_to_all(send_state, "dp", split_axis=0, concat_axis=0, tiled=True),
        lax.all_to_all(send_cache, "dp", split_axis=0, concat_axis=0, tiled=True),
    )
    state_in = got_state[sender]
    cache_in = got_cache[sender]
    slot_line = jnp.arange(slot_count)
    gone = jnp.any(slot_line[:, None] == leaving_slot[None, :], axis=1)
    new_states = jnp.where(gone[:, None, None], jnp.zeros_like(states), states)
    block_line = jnp.arange(block_count)
    gone_blocks = jnp.any(block_line[:, None, None] == leaving_block[None], axis=(1, 2))
    new_cache = jnp.where(gone_blocks[:, None, None, None], jnp.zeros_like(kv_blocks), kv_blocks)
    for move_index in range(moves):
        anchor = sender[move_index]
        place = plan_slots[anchor, move_index, 2]
        landing = (slot_line == place) & arriving[move_index]
        new_states = jnp.where(landing[:, None, None], state_in[move_index][None], new_states)
        for block_index in range(per_request):
            spot = plan_blocks[anchor, move_index, 1, block_index]
            block_hit = (block_line == spot) & arriving[move_index]
            new_cache = jnp.where(
                block_hit[:, None, None, None], cache_in[move_index, block_index][None], new_cache
            )
    experts = router.shape[1]
    tok_count = tokens.shape[0]
    width = tokens.shape[1]
    group = ranks // experts
    flat_ids = expert_ids.reshape(-1)
    onehot = (flat_ids[:, None] == jnp.arange(experts)[None, :]).astype(jnp.int32)
    earlier = jnp.cumsum(onehot, axis=0) - onehot
    slot_of = jnp.sum(earlier * onehot, axis=1)
    target_row = flat_ids * CAP + slot_of
    placer = (jnp.arange(experts * CAP)[:, None] == target_row[None, :]).astype(jnp.bfloat16)
    doubled = jnp.repeat(tokens, 2, axis=0)
    packed = jnp.dot(placer, doubled, preferred_element_type=jnp.float32).astype(jnp.bfloat16)
    outgoing = jnp.repeat(packed.reshape(experts, CAP, width), group, axis=0)
    incoming = lax.all_to_all(outgoing, "dp", split_axis=0, concat_axis=0, tiled=True)
    rows_in = incoming.reshape(ranks * CAP, width)
    piece = lax.all_gather(rows_in, "ep", axis=0, tiled=True)
    gate = jnp.dot(piece, w_gate[0], preferred_element_type=jnp.float32)
    upper = jnp.dot(piece, w_up[0], preferred_element_type=jnp.float32)
    hidden = (jax.nn.silu(gate) * upper).astype(jnp.bfloat16)
    summed = lax.psum_scatter(
        jnp.dot(hidden, w_down[0], preferred_element_type=jnp.float32),
        "ep",
        scatter_dimension=0,
        tiled=True,
    )
    returned = lax.all_to_all(
        summed.reshape(ranks, CAP, width), "dp", split_axis=0, concat_axis=0, tiled=True
    )
    expert_out = jnp.sum(returned.reshape(experts, group, CAP, width), axis=1).reshape(
        experts * CAP, width
    )
    chosen = expert_out[target_row].reshape(tok_count, 2, width)
    logits = jnp.dot(tokens.astype(jnp.float32), router, precision=lax.Precision.HIGHEST)
    scores = jax.nn.sigmoid(jnp.take_along_axis(logits, expert_ids, axis=1))
    weights = scores / jnp.sum(scores, axis=1, keepdims=True)
    mixed = jnp.sum(weights[:, :, None] * chosen, axis=1).astype(jnp.bfloat16)
    return (mixed, new_states, new_cache)


def solution(mesh):
    placed = (
        P(("dp", "ep"), None),
        P(),
        P(("dp", "ep"), None),
        P("dp", None, "ep"),
        P("dp", None, "ep"),
        P("dp", "ep", None),
        P("dp", None, "ep"),
        P("dp", None, None, "ep"),
        P(),
        P(),
        P(),
    )
    def step(*args):
        ranks, quads = lax.axis_size("dp"), lax.axis_size("ep")
        one_slab = args[1].shape[1] == ranks and ranks & (ranks - 1) == 0
        two_by_two = quads == 2 * 2
        return (fused if one_slab and two_by_two else local)(*args)

    return jax.shard_map(
        step,
        mesh=mesh,
        in_specs=placed,
        out_specs=(P(("dp", "ep"), None), P("dp", None, "ep"), P("dp", None, None, "ep")),
        check_vma=False,
    )
```
